8 devices in a mesh: dp: 2 (over y, z), tp: 4 (over x, core).
Axes of the slice: x: 2, y: 2, z: 1, core: 2. Of those that a mesh axis runs over, the one named last changes fastest.
Arguments:
- x: bfloat16 [2048, 4608], P(('dp', 'tp')), parts along dimension 0
- dy: bfloat16 [2048, 4608], P(('dp', 'tp')), parts along dimension 0
- gain: bfloat16 [4608], replicated
- wq: bfloat16 [4608, 4096], P(None, 'tp')
- wk: bfloat16 [4608, 2048], P(None, 'tp')
- wv: bfloat16 [4608, 2048], P(None, 'tp')
- wo: bfloat16 [4096, 4608], P('tp')
Outputs:
- output 1: bfloat16 [2048, 4608], P(('dp', 'tp')), parts along dimension 0
- output 2: float32 [2, 4608], P('dp'), parts along dimension 0
- output 3: bfloat16 [9216, 4096], P('dp', 'tp'), parts along dimension 0
- output 4: bfloat16 [9216, 2048], P('dp', 'tp'), parts along dimension 0
- output 5: bfloat16 [9216, 2048], P('dp', 'tp'), parts along dimension 0
- output 6: bfloat16 [8192, 4608], P(('dp', 'tp')), parts along dimension 0
There are 2 independent parts. The reference program is written for one: setup_inputs(seed, part) draws one part's arguments, and reference() takes and returns one part's arrays. A program takes and returns all parts, laid end to end along the dimension named above; an argument that names none is the same for every part.
All inputs are finite; a program needn't handle non-finite values.
Results may differ from the reference program's by a relative error of at most 0.018.
Values are sent between devices in bfloat16 or wider.
A program may use at most 2 GiB of HBM per device.

```python
import jax
import jax.numpy as jnp
from jax import lax

ROWS = 1024
D = 4608
HEADS = 32
KV_HEADS = 16
HEAD = 128
THETA = 10000


def setup_inputs(seed: int = 0, part: int = 0) -> dict:
    kx, ky, kn, kq, kk, kv, ko = jax.random.split(jax.random.key(seed), 7)

    def weights(key, rows, columns):
        return jax.random.normal(key, (rows, columns), jnp.float32) * rows**-0.5

    drawn = {
        "x": jax.random.normal(jax.random.fold_in(kx, part), (ROWS, D), jnp.float32),
        "dy": jax.random.normal(jax.random.fold_in(ky, part), (ROWS, D), jnp.float32) * ROWS**-0.5,
        "gain": 1 + 0.1 * jax.random.normal(kn, (D,), jnp.float32),
        "wq": 2 * weights(kq, D, HEADS * HEAD),
        "wk": 2 * weights(kk, D, KV_HEADS * HEAD),
        "wv": 4 * weights(kv, D, KV_HEADS * HEAD),
        "wo": weights(ko, HEADS * HEAD, D),
    }
    return {k: v.astype(jnp.bfloat16) for k, v in drawn.items()}


def normed(x, gain):
    wide = x.astype(jnp.float32)
    scale = lax.rsqrt(jnp.mean(wide * wide, -1, keepdims=True) + 1e-6)
    return (wide * scale * gain.astype(jnp.float32)).astype(jnp.bfloat16)


def turned(t, place, theta):
    half = t.shape[-1] // 2
    angle = place.astype(jnp.float32)[:, None] * theta ** (-jnp.arange(half, dtype=jnp.float32) / half)
    cos, sin = jnp.cos(angle)[:, None], jnp.sin(angle)[:, None]
    a, b = t[..., :half].astype(jnp.float32), t[..., half:].astype(jnp.float32)
    return jnp.concatenate([a * cos - b * sin, b * cos + a * sin], -1).astype(jnp.bfloat16)


def matmul(a, w):
    return jnp.dot(a, w, preferred_element_type=jnp.float32).astype(jnp.bfloat16)


def einsum(form, a, b):
    return jnp.einsum(form, a.astype(jnp.float32), b.astype(jnp.float32))


def attention(q, k, v):
    scores = einsum("tgsd,ugd->gstu", q, k) * q.shape[-1] ** -0.5
    token = jnp.arange(q.shape[0])
    scores = jnp.where(token[:, None] >= token, scores, -jnp.inf)
    weights = jax.nn.softmax(scores, -1).astype(jnp.bfloat16)
    return einsum("gstu,ugd->tgsd", weights, v).astype(jnp.bfloat16)


def forward(x, gain, wq, wk, wv, wo):
    rows = x.shape[0]
    a, place = normed(x, gain), jnp.arange(rows)
    k = turned(matmul(a, wk).reshape(rows, -1, HEAD), place, THETA)
    q = turned(matmul(a, wq).reshape(rows, -1, HEAD), place, THETA).reshape(rows, k.shape[1], -1, HEAD)
    v = matmul(a, wv).reshape(rows, -1, HEAD)
    seen = attention(q, k, v).reshape(rows, -1)
    return (x.astype(jnp.float32) + jnp.dot(seen, wo, preferred_element_type=jnp.float32)).astype(jnp.bfloat16)


def reference(x, dy, gain, wq, wk, wv, wo):
    _, back = jax.vjp(forward, x, gain.astype(jnp.float32), wq, wk, wv, wo)
    by_x, by_gain, *by_weights = back(dy)
    return (by_x, by_gain[None], *by_weights)
```

```python
import functools

import jax
import jax.numpy as jnp
from jax import lax
from jax.experimental import pallas as pl
from jax.experimental.pallas import tpu as pltpu

from jax.sharding import PartitionSpec as P

NEG = -1e30
LOG2E = 1.4426950408889634
VMEM = 67043328
HEAD = 128
THETA = 10000
BLOCK = 256


def _params(*semantics):
    return pltpu.CompilerParams(dimension_semantics=semantics, vmem_limit_bytes=VMEM)


def _estimate(flops, *arrays):
    return pl.CostEstimate(flops=flops, transcendentals=0, bytes_accessed=sum(a.size * a.dtype.itemsize for a in arrays))


def _sds(shape, dtype=jnp.bfloat16):
    return jax.ShapeDtypeStruct(shape, dtype)


ANY = pl.BlockSpec(memory_space=pl.ANY)


def _norm_kernel(x_ref, gain_ref, a_ref):
    wide = x_ref[...].astype(jnp.float32)
    scale = lax.rsqrt(jnp.mean(wide * wide, -1, keepdims=True) + 1e-6)
    a_ref[...] = (wide * scale * gain_ref[...].astype(jnp.float32)).astype(a_ref.dtype)


def normed(x, gain):
    rows, d = x.shape
    step = 64
    return pl.pallas_call(
        _norm_kernel,
        grid=(rows // step,),
        in_specs=[pl.BlockSpec((step, d), lambda i: (i, 0)), pl.BlockSpec((1, d), lambda i: (0, 0))],
        out_specs=pl.BlockSpec((step, d), lambda i: (i, 0)),
        out_shape=_sds((rows, d)),
        compiler_params=_params("arbitrary"),
        cost_estimate=_estimate(8 * x.size, x, x),
    )(x, gain)


def _turn(t, cos, sin):
    return t * cos + pltpu.roll(t, HEAD // 2, 1) * sin


def _unturn(t, cos, sin):
    return t * cos - pltpu.roll(t, HEAD // 2, 1) * sin


def _proj_kernel(ids, a0, a1, wq, wk, wv, cos_ref, sin_ref, *rest, nq, nk):
    q_ref, k_ref, v_ref = rest[-3:]
    n = pl.program_id(0)
    core = ids[1]

    def tile(w_ref, out_ref, turned):
        for a_ref, place in ((a0, core), (a1, 1 - core)):
            got = jnp.dot(a_ref[...], w_ref[...], preferred_element_type=jnp.float32)
            rows = pl.ds(pl.multiple_of(place * BLOCK, BLOCK), BLOCK)
            for h in range(2):
                t = got[:, h * HEAD : (h + 1) * HEAD]
                if turned:
                    t = _turn(t.astype(jnp.bfloat16).astype(jnp.float32), cos_ref[rows, :], sin_ref[rows, :])
                out_ref[h, rows, :] = t.astype(jnp.bfloat16)

    @pl.when(n < nq)
    def _():
        tile(wq, q_ref, True)

    @pl.when((n >= nq) & (n < nq + nk))
    def _():
        tile(wk, k_ref, True)

    @pl.when(n >= nq + nk)
    def _():
        tile(wv, v_ref, False)


def project(ids, chip, a0, a1, wq, wk, wv, cos, sin, kept=()):
    d = a0.shape[1]
    wide = 2 * HEAD
    nq, nk, nv = (w.shape[1] // wide for w in (wq, wk, wv))
    heads, kv = wq.shape[1] // HEAD, wk.shape[1] // HEAD
    whole = pl.BlockSpec((BLOCK, d), lambda n, ids: (0, 0))

    def at(first, count):
        return lambda n, ids: (0, jnp.clip(n - first, 0, count - 1))

    def out(first, count):
        return lambda n, ids: (jnp.clip(n - first, 0, count - 1), ids[chip], 0)

    table = pl.BlockSpec((2 * BLOCK, HEAD), lambda n, ids: (ids[chip], 0))
    return pl.pallas_call(
        functools.partial(_proj_kernel, nq=nq, nk=nk),
        grid_spec=pltpu.PrefetchScalarGridSpec(
            num_scalar_prefetch=1,
            grid=(nq + nk + nv,),
            in_specs=[whole, whole, pl.BlockSpec((d, wide), at(0, nq)), pl.BlockSpec((d, wide), at(nq, nk)),
                      pl.BlockSpec((d, wide), at(nq + nk, nv)), table, table, *([ANY] * len(kept))],
            out_specs=[pl.BlockSpec((2, 2 * BLOCK, HEAD), lambda n, ids: (jnp.minimum(n, nq - 1), 0, 0)),
                       pl.BlockSpec((2, 2 * BLOCK, HEAD), out(nq, nk)), pl.BlockSpec((2, 2 * BLOCK, HEAD), out(nq + nk, nv))],
        ),
        out_shape=[_sds((heads, 2 * BLOCK, HEAD)), _sds((kv, 4 * BLOCK, HEAD)), _sds((kv, 4 * BLOCK, HEAD))],
        input_output_aliases={8: 1, 9: 2} if kept else {},
        compiler_params=_params("arbitrary"),
        cost_estimate=_estimate(4 * BLOCK * d * (wq.shape[1] + 2 * wk.shape[1]), a0, a1, wq, wk, wv),
    )(ids, a0, a1, wq, wk, wv, cos, sin, *kept)


def _nt(a, b):
    return lax.dot_general(a, b, (((1,), (1,)), ((), ())), preferred_element_type=jnp.float32)


def _dseen_own_kernel(ids, y0, y1, wo, out_ref):
    core = ids[1]
    for y_ref, place in ((y0, core), (y1, 1 - core)):
        got = _nt(y_ref[...], wo[...]).astype(jnp.bfloat16)
        rows = pl.ds(pl.multiple_of(place * BLOCK, BLOCK), BLOCK)
        for h in range(2):
            out_ref[h, rows, :] = got[:, h * HEAD : (h + 1) * HEAD]


def dseen_own(ids, y0, y1, wo):
    k, d = wo.shape
    whole = pl.BlockSpec((BLOCK, d), lambda n, ids: (0, 0))
    return pl.pallas_call(
        _dseen_own_kernel,
        grid_spec=pltpu.PrefetchScalarGridSpec(
            num_scalar_prefetch=1,
            grid=(k // (2 * HEAD),),
            in_specs=[whole, whole, pl.BlockSpec((2 * HEAD, d), lambda n, ids: (n, 0))],
            out_specs=pl.BlockSpec((2, 2 * BLOCK, HEAD), lambda n, ids: (n, 0, 0)),
        ),
        out_shape=_sds((k // HEAD, 2 * BLOCK, HEAD)),
        compiler_params=_params("arbitrary"),
        cost_estimate=_estimate(4 * BLOCK * d * k, y0, y1, wo),
    )(ids, y0, y1, wo)


def _dseen_half_kernel(ids, r_ref, f_ref, wr, wf, out_ref):
    got = (_nt(r_ref[...], wr[...]) + _nt(f_ref[...], wf[...])).astype(jnp.bfloat16)
    for h in range(2):
        out_ref[h] = got[:, h * HEAD : (h + 1) * HEAD]


def dseen_remote(ids, r, f, wo):
    k, d = wo.shape
    whole = pl.BlockSpec((BLOCK, d // 2), lambda n, ids: (0, 0))
    return pl.pallas_call(
        _dseen_half_kernel,
        grid_spec=pltpu.PrefetchScalarGridSpec(
            num_scalar_prefetch=1,
            grid=(k // (2 * HEAD),),
            in_specs=[whole, whole, pl.BlockSpec((2 * HEAD, d // 2), lambda n, ids: (n, 1 - ids[1])),
                      pl.BlockSpec((2 * HEAD, d // 2), lambda n, ids: (n, ids[1]))],
            out_specs=pl.BlockSpec((2, BLOCK, HEAD), lambda n, ids: (n, 0, 0)),
        ),
        out_shape=_sds((k // HEAD, BLOCK, HEAD)),
        compiler_params=_params("arbitrary"),
        cost_estimate=_estimate(2 * BLOCK * d * k, r, f, wo),
    )(ids, r, f, wo, wo)


def _dot(a, b, ca, cb):
    return lax.dot_general(a, b, (((ca,), (cb,)), ((), ())), preferred_element_type=jnp.float32)


def _causal():
    shape = (BLOCK, 2 * BLOCK)
    return lax.rem(lax.broadcasted_iota(jnp.int32, shape, 1), BLOCK) >= lax.broadcasted_iota(jnp.int32, shape, 0)


def _see_kernel(ids, q_ref, k_ref, v_ref, out_ref, lse_ref, top_s, mix_s, *, base, scale):
    kb = k_ref.shape[0]
    e = scale * LOG2E
    cols = 2 * BLOCK
    top_s[...] = jnp.full_like(top_s, NEG)
    mix_s[...] = jnp.zeros_like(mix_s)
    ones = jnp.ones((8, BLOCK), jnp.bfloat16)
    qs = [q_ref[2 * i : 2 * i + 2].reshape(cols, HEAD) for i in range(kb)]

    def block(j, masked):
        here = pl.ds(pl.multiple_of(j * BLOCK, BLOCK), BLOCK)
        scores = [_nt(k_ref[i, here, :], qs[i]) for i in range(kb)]
        if masked:
            scores = [jnp.where(_causal(), s, 2 * NEG) for s in scores]
        for i, s in enumerate(scores):
            old = top_s[i : i + 1]
            top = jnp.maximum(old, s.max(axis=0, keepdims=True))
            top_s[i : i + 1] = top
            p = jnp.exp2((s - top) * e).astype(jnp.bfloat16)
            values = jnp.concatenate([v_ref[i, here, :].T, ones], axis=0)
            mix_s[i] = mix_s[i] * jnp.exp2((old - top) * e) + _dot(values, p, 1, 0)

    last = base(ids) + pl.program_id(1)
    lax.fori_loop(0, last, lambda j, _: block(j, False), None)
    block(last, True)
    for i in range(kb):
        total = mix_s[i, HEAD : HEAD + 1]
        out_ref[2 * i : 2 * i + 2] = (mix_s[i, :HEAD] * (1 / total)).T.reshape(2, BLOCK, HEAD).astype(jnp.bfloat16)
        lse = top_s[i : i + 1] * scale + jnp.log(total)
        for h in range(2):
            lse_ref[i, h : h + 1] = lse[:, h * BLOCK : (h + 1) * BLOCK]


def see(ids, base, q, k, v):
    kv, sk, _ = k.shape
    kb = 4
    count = q.shape[1] // BLOCK
    queries = pl.BlockSpec((2 * kb, BLOCK, HEAD), lambda g, i, ids: (g, i, 0))
    keys = pl.BlockSpec((kb, sk, HEAD), lambda g, i, ids: (g, 0, 0))
    return pl.pallas_call(
        functools.partial(_see_kernel, base=base, scale=HEAD**-0.5),
        grid_spec=pltpu.PrefetchScalarGridSpec(
            num_scalar_prefetch=1,
            grid=(kv // kb, count),
            in_specs=[queries, keys, keys],
            out_specs=[queries, pl.BlockSpec((kb, 2, BLOCK), lambda g, i, ids: (g, 0, i))],
            scratch_shapes=[pltpu.VMEM((kb, 2 * BLOCK), jnp.float32), pltpu.VMEM((kb, HEAD + 8, 2 * BLOCK), jnp.float32)],
        ),
        out_shape=[_sds(q.shape), _sds((kv, 2, q.shape[1]), jnp.float32)],
        compiler_params=_params("arbitrary", "arbitrary"),
        cost_estimate=_estimate(4 * q.shape[1] * sk * HEAD * 2 * kv, q, k, v),
    )(ids, q, k, v)


def _bwd_kernel(ids, q_ref, k_ref, v_ref, do_ref, o_ref, lse_ref, cos_ref, sin_ref, *rest, base, scale, carried):
    dk_in, dv_in = rest[:2] if carried else (None, None)
    dq_ref, dk_ref, dv_ref, dq_s = rest[-4:]
    kb = k_ref.shape[0]
    iq = pl.program_id(1)
    e = scale * LOG2E
    cols = 2 * BLOCK

    @pl.when(iq == 0)
    def _():
        dk_ref[...] = dk_in[...] if carried else jnp.zeros_like(dk_ref)
        dv_ref[...] = dv_in[...] if carried else jnp.zeros_like(dv_ref)

    dq_s[...] = jnp.zeros_like(dq_s)
    qs, dos, deltas, lses = [], [], [], []
    for i in range(kb):
        q2 = q_ref[2 * i : 2 * i + 2].reshape(cols, HEAD)
        do2 = do_ref[2 * i : 2 * i + 2].reshape(cols, HEAD)
        o2 = o_ref[2 * i : 2 * i + 2].reshape(cols, HEAD)
        both = do2.astype(jnp.float32) * o2.astype(jnp.float32)
        qs.append(q2)
        dos.append(do2)
        deltas.append(both.T.sum(0, keepdims=True))
        lses.append(jnp.concatenate([lse_ref[i, 0:1, :], lse_ref[i, 1:2, :]], axis=1) * LOG2E)

    def block(j, masked):
        here = pl.ds(pl.multiple_of(j * BLOCK, BLOCK), BLOCK)
        scores = [_nt(k_ref[i, here, :], qs[i]) for i in range(kb)]
        dps = [_nt(v_ref[i, here, :], dos[i]) for i in range(kb)]
        if masked:
            ok = _causal()
        for i in range(kb):
            p = jnp.exp2(scores[i] * e - lses[i])
            if masked:
                p = jnp.where(ok, p, 0.0)
            ds = (p * (dps[i] - deltas[i])).astype(jnp.bfloat16)
            dv_ref[i, here, :] += _dot(p.astype(jnp.bfloat16), dos[i], 1, 0)
            dk_ref[i, here, :] += _dot(ds, qs[i], 1, 0)
            dq_s[i] += _dot(k_ref[i, here, :].T, ds, 1, 0)

    last = base(ids) + iq
    lax.fori_loop(0, last, lambda j, _: block(j, False), None)
    block(last, True)
    for i in range(kb):
        got = (dq_s[i] * scale).T
        for h in range(2):
            t = _unturn(got[h * BLOCK : (h + 1) * BLOCK].astype(jnp.bfloat16).astype(jnp.float32), cos_ref[...], sin_ref[...])
            dq_ref[:, (2 * i + h) * HEAD : (2 * i + h + 1) * HEAD] = t.astype(jnp.bfloat16)


def backward(ids, base, skip, count, q, k, v, d_out, out, lse, cos, sin, carry=()):
    kv, sk, _ = k.shape
    kb = 2
    queries = pl.BlockSpec((2 * kb, BLOCK, HEAD), lambda g, i, ids: (g, skip + i, 0))
    keys = pl.BlockSpec((kb, sk, HEAD), lambda g, i, ids: (g, 0, 0))
    table = pl.BlockSpec((BLOCK, HEAD), lambda g, i, ids: (base(ids) + i, 0))
    return pl.pallas_call(
        functools.partial(_bwd_kernel, base=base, scale=HEAD**-0.5, carried=bool(carry)),
        grid_spec=pltpu.PrefetchScalarGridSpec(
            num_scalar_prefetch=1,
            grid=(kv // kb, count),
            in_specs=[queries, keys, keys, pl.BlockSpec((2 * kb, BLOCK, HEAD), lambda g, i, ids: (g, i, 0)), queries,
                      pl.BlockSpec((kb, 2, BLOCK), lambda g, i, ids: (g, 0, skip + i)), table, table, *([keys] * len(carry))],
            out_specs=[pl.BlockSpec((BLOCK, 2 * kb * HEAD), lambda g, i, ids: (i, g)), keys, keys],
            scratch_shapes=[pltpu.VMEM((kb, HEAD, 2 * BLOCK), jnp.float32)],
        ),
        out_shape=[_sds((count * BLOCK, 2 * kv * HEAD)), _sds(k.shape, jnp.float32), _sds(k.shape, jnp.float32)],
        compiler_params=_params("arbitrary", "arbitrary"),
        cost_estimate=_estimate(10 * count * BLOCK * sk * HEAD * 2 * kv, q, k, v, d_out, out),
    )(ids, q, k, v, d_out, out, lse, cos, sin, *carry)


WIDE = 768


def _dkv(dk_ref, dv_ref, cos_ref, sin_ref):
    scale = HEAD**-0.5
    parts = [_unturn((dk_ref[i] * scale).astype(jnp.bfloat16).astype(jnp.float32), cos_ref[...], sin_ref[...]).astype(jnp.bfloat16)
             for i in range(dk_ref.shape[0])]
    parts += [dv_ref[i].astype(jnp.bfloat16) for i in range(dv_ref.shape[0])]
    return jnp.concatenate(parts, axis=1)


def _term(dq, dkv, wq, wk, wv):
    half = dkv.shape[1] // 2
    return _nt(dq, wq[...]) + _nt(dkv[:, :half], wk[...]) + _nt(dkv[:, half:], wv[...])


def _give_kernel(ids, dq_ref, dk_ref, dv_ref, cos_ref, sin_ref, wq, wk, wv, out_ref, dkv_ref):
    @pl.when(pl.program_id(0) == 0)
    def _():
        dkv_ref[...] = _dkv(dk_ref, dv_ref, cos_ref, sin_ref)

    out_ref[...] = _term(dq_ref[...], dkv_ref[...], wq, wk, wv).astype(jnp.bfloat16)


def _weight_tiles(wq, wk, wv, tile):
    return [pl.BlockSpec((WIDE, w.shape[1]), lambda n, ids: (tile(n, ids), 0)) for w in (wq, wk, wv)]


def give(ids, block, dq, dk, dv, cos, sin, wq, wk, wv):
    d = wq.shape[0]
    steps = d // 2 // WIDE
    width = dq.shape[1]
    keys = pl.BlockSpec((dk.shape[0], BLOCK, HEAD), lambda n, ids: (0, ids[block], 0))
    table = pl.BlockSpec((BLOCK, HEAD), lambda n, ids: (ids[block], 0))
    return pl.pallas_call(
        _give_kernel,
        grid_spec=pltpu.PrefetchScalarGridSpec(
            num_scalar_prefetch=1,
            grid=(steps,),
            in_specs=[pl.BlockSpec((BLOCK, width), lambda n, ids: (0, 0)), keys, keys, table, table,
                      *_weight_tiles(wq, wk, wv, lambda n, ids: ids[1] * steps + n)],
            out_specs=[pl.BlockSpec((BLOCK, WIDE), lambda n, ids: (0, n)), pl.BlockSpec((BLOCK, width), lambda n, ids: (0, 0))],
        ),
        out_shape=[_sds((BLOCK, d // 2)), _sds((BLOCK, width))],
        compiler_params=_params("arbitrary"),
        cost_estimate=_estimate(2 * BLOCK * d * width, wq, wk, wv),
    )(ids, dq, dk, dv, cos, sin, wq, wk, wv)


def _keep_kernel(ids, dq_ref, dkv_ref, other_ref, wq, wk, wv, out_ref):
    out_ref[...] = (_term(dq_ref[...], dkv_ref[...], wq, wk, wv) + other_ref[...].astype(jnp.float32)).astype(jnp.bfloat16)


def keep(ids, dq, dkv, other, wq, wk, wv):
    d = wq.shape[0]
    steps = d // 2 // WIDE
    width = dq.shape[1]
    whole = pl.BlockSpec((BLOCK, width), lambda n, ids: (0, 0))
    part = pl.BlockSpec((BLOCK, WIDE), lambda n, ids: (0, n))
    return pl.pallas_call(
        _keep_kernel,
        grid_spec=pltpu.PrefetchScalarGridSpec(
            num_scalar_prefetch=1,
            grid=(steps,),
            in_specs=[whole, whole, part, *_weight_tiles(wq, wk, wv, lambda n, ids: (1 - ids[1]) * steps + n)],
            out_specs=part,
        ),
        out_shape=_sds((BLOCK, d // 2)),
        compiler_params=_params("arbitrary"),
        cost_estimate=_estimate(2 * BLOCK * d * width, wq, wk, wv),
    )(ids, dq, dkv, other, wq, wk, wv)


def _own_kernel(ids, dq_ref, dk_ref, dv_ref, cos_ref, sin_ref, wq, wk, wv, mine_ref, other_ref, dkv_ref):
    @pl.when(pl.program_id(0) == 0)
    def _():
        dkv_ref[...] = _dkv(dk_ref, dv_ref, cos_ref, sin_ref)

    for out_ref, place in ((mine_ref, ids[1]), (other_ref, 1 - ids[1])):
        rows = pl.ds(pl.multiple_of(place * BLOCK, BLOCK), BLOCK)
        out_ref[...] = _term(dq_ref[rows, :], dkv_ref[rows, :], wq, wk, wv).astype(out_ref.dtype)


def own_terms(ids, dq, dk, dv, cos, sin, wq, wk, wv):
    d = wq.shape[0]
    width = dq.shape[1]
    keys = pl.BlockSpec((dk.shape[0], 2 * BLOCK, HEAD), lambda n, ids: (0, ids[2], 0))
    table = pl.BlockSpec((2 * BLOCK, HEAD), lambda n, ids: (ids[2], 0))
    whole = pl.BlockSpec((2 * BLOCK, width), lambda n, ids: (0, 0))
    part = pl.BlockSpec((BLOCK, WIDE), lambda n, ids: (0, n))
    return pl.pallas_call(
        _own_kernel,
        grid_spec=pltpu.PrefetchScalarGridSpec(
            num_scalar_prefetch=1,
            grid=(d // WIDE,),
            in_specs=[whole, keys, keys, table, table, *_weight_tiles(wq, wk, wv, lambda n, ids: n)],
            out_specs=[part, part, whole],
        ),
        out_shape=[_sds((BLOCK, d), jnp.float32), _sds((BLOCK, d)), _sds((2 * BLOCK, width))],
        compiler_params=_params("arbitrary"),
        cost_estimate=_estimate(8 * BLOCK * d * width, wq, wk, wv),
    )(ids, dq, dk, dv, cos, sin, wq, wk, wv)


def _dw_kernel(ids, a0, a1, a2, a3, q0, q1, q2, e0, e1, e2, oq, ok, ov, all_s):
    core = ids[1]
    half = q0.shape[1]

    @pl.when(pl.program_id(0) == 0)
    def _():
        def put(slot, q, e):
            rows = pl.ds(pl.multiple_of(slot * BLOCK, BLOCK), BLOCK)
            all_s[rows, :half] = q
            all_s[rows, half:] = e

        put(core, q0[:BLOCK, :], e0[:BLOCK, :])
        put(1 - core, q0[BLOCK:, :], e0[BLOCK:, :])
        put(3 - core, q1[...], e1[...])
        put(2 + core, q2[...], e2[...])

    a = jnp.concatenate([a0[...], a1[...], a2[...], a3[...]], axis=0)
    at = a.T
    nq, nk = oq.shape[1], ok.shape[1]
    for first, out_ref in ((0, oq), (nq, ok), (nq + nk, ov)):
        out_ref[...] = jnp.dot(at, all_s[:, first : first + out_ref.shape[1]], preferred_element_type=jnp.float32).astype(jnp.bfloat16)


def weight_grads(ids, states, dqs, dkvs, nk):
    d = states[0].shape[1]
    nq = dqs[0].shape[1]
    wide = 512
    whole = lambda a: pl.BlockSpec(a.shape, lambda n, ids: (0, 0))
    outs = (nq, nk, nk)
    return pl.pallas_call(
        _dw_kernel,
        grid_spec=pltpu.PrefetchScalarGridSpec(
            num_scalar_prefetch=1,
            grid=(d // wide,),
            in_specs=[*[pl.BlockSpec((BLOCK, wide), lambda n, ids: (0, n)) for _ in states], *[whole(a) for a in (*dqs, *dkvs)]],
            out_specs=[pl.BlockSpec((wide, n), lambda i, ids: (i, 0)) for n in outs],
            scratch_shapes=[pltpu.VMEM((4 * BLOCK, nq + 2 * nk), jnp.bfloat16)],
        ),
        out_shape=[_sds((d, n)) for n in outs],
        compiler_params=_params("arbitrary"),
        cost_estimate=_estimate(8 * BLOCK * d * (nq + 2 * nk), *states, *dqs, *dkvs),
    )(ids, *states, *dqs, *dkvs)


def _dwo_kernel(ids, s_own, s_rem, y0, y1, hr, hf, lr, lf, out_ref, t_s):
    core = ids[1]
    n = pl.program_id(0)

    @pl.when(n == 0)
    def _():
        for h in range(s_own.shape[0]):
            mine = s_own[h, pl.ds(pl.multiple_of(core * BLOCK, BLOCK), BLOCK), :]
            other = s_own[h, pl.ds(pl.multiple_of((1 - core) * BLOCK, BLOCK), BLOCK), :]
            rows = jnp.concatenate([mine, other, s_rem[h, BLOCK:, :], s_rem[h, :BLOCK, :]], axis=0)
            t_s[h * HEAD : (h + 1) * HEAD, :] = rows.T

    first = n < pl.num_programs(0) // 2
    high = jnp.where(first, hr[...], hf[...])
    low = jnp.where(first, lr[...], lf[...])
    y = jnp.concatenate([y0[...], y1[...], high, low], axis=0)
    out_ref[...] = jnp.dot(t_s[...], y, preferred_element_type=jnp.float32).astype(jnp.bfloat16)


def wo_grad(ids, seen_own, seen_rem, y0, y1, hr, hf, lr, lf):
    d = y0.shape[1]
    steps = d // WIDE
    half = steps // 2
    rows = seen_own.shape[0] * HEAD

    def at(n, ids):
        return 0, lax.rem(n + (1 - ids[1]) * half, steps)

    r = pl.BlockSpec((BLOCK, WIDE), lambda n, ids: (0, jnp.minimum(n, half - 1)))
    f = pl.BlockSpec((BLOCK, WIDE), lambda n, ids: (0, jnp.maximum(n - half, 0)))
    seen = pl.BlockSpec(seen_own.shape, lambda n, ids: (0, 0, 0))
    y = pl.BlockSpec((BLOCK, WIDE), at)
    return pl.pallas_call(
        _dwo_kernel,
        grid_spec=pltpu.PrefetchScalarGridSpec(
            num_scalar_prefetch=1,
            grid=(steps,),
            in_specs=[seen, seen, y, y, r, f, r, f],
            out_specs=pl.BlockSpec((rows, WIDE), at),
            scratch_shapes=[pltpu.VMEM((rows, 4 * BLOCK), jnp.bfloat16)],
        ),
        out_shape=_sds((rows, d)),
        compiler_params=_params("arbitrary"),
        cost_estimate=_estimate(8 * BLOCK * d * rows, seen_own, seen_rem, y0, y1, hr, hf, lr, lf),
    )(ids, seen_own, seen_rem, y0, y1, hr, hf, lr, lf)


def _finish_kernel(ids, x_ref, dy_ref, gain_ref, mine_ref, other_ref, rh, rl, fh, fl, dx_ref, dgain_ref):
    upper = ids[1] == 1
    left = jnp.where(upper, rh[...], fl[...])
    right = jnp.where(upper, fh[...], rl[...])
    da = mine_ref[...] + other_ref[...].astype(jnp.float32) + jnp.concatenate([left, right], axis=1).astype(jnp.float32)
    x = x_ref[...].astype(jnp.float32)
    scale = lax.rsqrt(jnp.mean(x * x, -1, keepdims=True) + 1e-6)
    hat = x * scale
    by_hat = da * gain_ref[...].astype(jnp.float32)
    dx = scale * (by_hat - hat * jnp.mean(by_hat * hat, -1, keepdims=True))
    dx_ref[...] = (dy_ref[...].astype(jnp.float32) + dx).astype(jnp.bfloat16)
    part = (da * hat).sum(0, keepdims=True)

    @pl.when(pl.program_id(0) == 0)
    def _():
        dgain_ref[...] = part

    @pl.when(pl.program_id(0) > 0)
    def _():
        dgain_ref[...] += part


def finish(ids, x, dy, gain, mine, other, rh, rl, fh, fl):
    rows, d = x.shape
    step = 64
    whole = pl.BlockSpec((step, d), lambda i, ids: (i, 0))
    half = pl.BlockSpec((step, d // 2), lambda i, ids: (i, 0))
    one = pl.BlockSpec((1, d), lambda i, ids: (0, 0))
    return pl.pallas_call(
        _finish_kernel,
        grid_spec=pltpu.PrefetchScalarGridSpec(
            num_scalar_prefetch=1,
            grid=(rows // step,),
            in_specs=[whole, whole, one, whole, whole, half, half, half, half],
            out_specs=[whole, one],
        ),
        out_shape=[_sds((rows, d)), _sds((1, d), jnp.float32)],
        compiler_params=_params("arbitrary"),
        cost_estimate=_estimate(20 * x.size, x, dy, mine, other),
    )(ids, x, dy, gain, mine, other, rh, rl, fh, fl)


def solution(mesh):
    across = [(i, i ^ 2) for i in range(4)]
    beside = [(i, i ^ 1) for i in range(4)]
    up = [(0, 1), (2, 3)]
    down = [(1, 0), (3, 2)]

    def send(a, pairs):
        return lax.ppermute(a, "tp", pairs)

    def body(x, dy, gain, wq, wk, wv, wo):
        d = x.shape[1]
        gain = gain[None]
        me = lax.axis_index("tp").astype(jnp.int32)
        core, chip = me % 2, me // 2
        ids = jnp.stack([me, core, chip, 1 - chip, 2 * (1 - chip) + 1, 2 * (1 - chip)])
        upper = core == 1
        a0 = normed(x, gain)
        a2 = send(a0, across)
        a1 = send(a0, beside)
        dy1 = send(dy, beside)
        hr = send(jnp.where(upper, dy[:, : d // 2], dy1[:, d // 2 :]), across)
        lr = send(jnp.where(upper, dy1[:, : d // 2], dy[:, d // 2 :]), across)
        a3 = send(a2, beside)
        hf = send(hr, beside)
        lf = send(lr, beside)

        half = HEAD // 2
        angle = jnp.arange(4 * BLOCK).astype(jnp.float32)[:, None] * THETA ** (-jnp.arange(half, dtype=jnp.float32) / half)
        cos, sin = jnp.cos(angle), jnp.sin(angle)
        cos, sin = jnp.concatenate([cos, cos], 1), jnp.concatenate([-sin, sin], 1)

        q_own, k, v = project(ids, 2, a0, a1, wq, wk, wv, cos, sin)
        ds_own = dseen_own(ids, dy, dy1, wo)
        q_rem, k, v = project(ids, 3, a2, a3, wq, wk, wv, cos, sin, (k, v))
        seen_own, lse_own = see(ids, lambda s: 2 * s[2], q_own, k, v)
        seen_rem, lse_rem = see(ids, lambda s: 2 * s[3], q_rem, k, v)
        dq_own, dk, dv = backward(ids, lambda s: 2 * s[2], 0, 2, q_own, k, v, ds_own, seen_own, lse_own, cos, sin)
        ds_h = dseen_remote(ids, hr, hf, wo)
        dq_h, dk, dv = backward(ids, lambda s: s[4], 1, 1, q_rem, k, v, ds_h, seen_rem, lse_rem, cos, sin, (dk, dv))
        give_h, dkv_h = give(ids, 4, dq_h, dk, dv, cos, sin, wq, wk, wv)
        sum_h = keep(ids, dq_h, dkv_h, send(give_h, beside), wq, wk, wv)
        rh = send(sum_h, across)
        ds_l = dseen_remote(ids, lr, lf, wo)
        dq_l, dk, dv = backward(ids, lambda s: s[5], 0, 1, q_rem, k, v, ds_l, seen_rem, lse_rem, cos, sin, (dk, dv))
        give_l, dkv_l = give(ids, 5, dq_l, dk, dv, cos, sin, wq, wk, wv)
        sum_l = keep(ids, dq_l, dkv_l, send(give_l, beside), wq, wk, wv)
        rl = send(sum_l, across)
        fh, fl = send(rh, up), send(rl, down)

        dq_own, seen_own, _ = lax.optimization_barrier((dq_own, seen_own, sum_l))
        mine, other, dkv_own = own_terms(ids, dq_own, dk, dv, cos, sin, wq, wk, wv)
        other = send(other, beside)
        dwo = wo_grad(ids, seen_own, seen_rem, dy, dy1, hr, hf, lr, lf)
        dwq, dwk, dwv = weight_grads(ids, (a0, a1, a2, a3), (dq_own, dq_h, dq_l), (dkv_own, dkv_h, dkv_l), wk.shape[1])
        dx, dgain = finish(ids, x, dy, gain, mine, other, rh, rl, fh, fl)
        dgain = dgain + send(dgain, beside)
        dgain = dgain + send(dgain, across)
        return dx, dgain, dwq, dwk, dwv, dwo

    tokens, columns = P(("dp", "tp"), None), P(None, "tp")
    return jax.shard_map(
        body,
        mesh=mesh,
        in_specs=(tokens, tokens, P(None), columns, columns, columns, P("tp", None)),
        out_specs=(tokens, P("dp", None), P("dp", "tp"), P("dp", "tp"), P("dp", "tp"), P(("dp", "tp"), None)),
        check_vma=False,
    )
```

```python
import jax
import jax.numpy as jnp
from jax import lax
from jax.experimental import pallas as pl
from jax.experimental.pallas import tpu as pltpu

from jax.sharding import PartitionSpec as P

NEG = -1e30
LOG2E = 1.4426950408889634
VMEM = 67043328
HEAD = 128
THETA = 10000
BLOCK = 256


def _params(*semantics):
    return pltpu.CompilerParams(dimension_semantics=semantics, vmem_limit_bytes=VMEM)


def _estimate(flops, *arrays):
    return pl.CostEstimate(flops=flops, transcendentals=0, bytes_accessed=sum(a.size * a.dtype.itemsize for a in arrays))


def _sds(shape, dtype=jnp.bfloat16):
    return jax.ShapeDtypeStruct(shape, dtype)


ANY = pl.BlockSpec(memory_space=pl.ANY)


def _dot(a, b, ca, cb):
    return lax.dot_general(a, b, (((ca,), (cb,)), ((), ())), preferred_element_type=jnp.float32)


def _nt(a, b):
    return _dot(a, b, 1, 1)


def _turn(t, cos, sin):
    return t * cos + pltpu.roll(t, HEAD // 2, 1) * sin


def _unturn(t, cos, sin):
    return t * cos - pltpu.roll(t, HEAD // 2, 1) * sin


def _causal():
    shape = (BLOCK, 2 * BLOCK)
    return lax.rem(lax.broadcasted_iota(jnp.int32, shape, 1), BLOCK) >= lax.broadcasted_iota(jnp.int32, shape, 0)


def _rows(block, size=BLOCK):
    return pl.ds(pl.multiple_of(block * size, size), size)


def _loop(first, last, body):
    lax.fori_loop(first, last, lambda i, _: body(i), None)


def _main_kernel(gain, cos, sin, x, dy, wq, wk, wv, wo,
                 a0_o, a1_o, a2_o, a3_o, y1_o, yr_o, yf_o, seen_o, dq_o, dkv_o, dk_o, dv_o, sumh_o, suml_o,
                 w_s, wo_s, st, qkv_s, do_s, o_s, lse_s, top_s, mix_s, dq_s, dk_s, dv_s, dqkv_s, give_s, got_s, keep_s,
                 lsem, ssem, rsem):
    dp, me = lax.axis_index("dp"), lax.axis_index("tp")
    core, chip = lax.rem(me, 2), lax.div(me, 2)
    beside, across = (dp, me + 1 - 2 * core), (dp, lax.rem(me + 2, 4))
    far = 1 - chip
    d = x.shape[1]
    half, part = d // 2, BLOCK // 2
    scale = HEAD**-0.5
    e = scale * LOG2E
    cols = 2 * BLOCK
    nh, kv = do_s.shape[0], dk_s.shape[0]
    MESH = pl.DeviceIdType.MESH

    barrier = pltpu.get_barrier_semaphore()
    for peer in (beside, across):
        pl.semaphore_signal(barrier, inc=1, device_id=peer, device_id_type=MESH)
    pl.semaphore_wait(barrier, 2)

    used = [0, 0]

    def local(src, dst):
        copy = pltpu.make_async_copy(src, dst, lsem.at[used[0]])
        used[0] += 1
        copy.start()
        return copy

    def away(src, dst, to, at):
        return pltpu.make_async_remote_copy(src_ref=src, dst_ref=dst, send_sem=ssem.at[at], recv_sem=rsem.at[at], device_id=to,
                                            device_id_type=MESH)

    def remote(src, dst, to):
        copy = away(src, dst, to, used[1])
        used[1] += 1
        copy.start()
        return copy

    parts = [pl.ds(j * part, part) for j in range(2)]
    y1 = remote(dy, y1_o, beside)
    xs = [local(x.at[r], st.at[0, r]) for r in parts]
    nq, nk = wq.shape[1], wk.shape[1]
    wo_in = local(wo, wo_s)
    w_in = [local(w, w_s.at[:, pl.ds(at, w.shape[1])]) for w, at in ((wq, 0), (wk, nq), (wv, nq + nk))]
    far_a, near_a = [], []
    for j in range(2):
        xs[j].wait()

        def norm(i):
            rows = pl.ds(pl.multiple_of(j * part + i * 16, 16), 16)
            wide = st[0, rows, :].astype(jnp.float32)
            inv = lax.rsqrt(jnp.mean(wide * wide, -1, keepdims=True) + 1e-6)
            st[1, rows, :] = (wide * inv * gain[...].astype(jnp.float32)).astype(jnp.bfloat16)

        _loop(0, part // 16, norm)
        local(st.at[1, parts[j]], a0_o.at[parts[j]]).wait()
        far_a.append(remote(a0_o.at[parts[j]], a2_o.at[parts[j]], across))
        near_a.append(remote(a0_o.at[parts[j]], a1_o.at[parts[j]], beside))

    y1.wait_recv()
    first, second = pl.ds(0, half), pl.ds(half, half)
    hl = used[1]
    on = hl + 2
    gv = hl + 4
    used[1] += 6

    @pl.when(core == 1)
    def _():
        away(dy.at[:, first], yr_o.at[0], across, hl).start()
        away(y1_o.at[:, first], yr_o.at[1], across, hl + 1).start()

    @pl.when(core == 0)
    def _():
        away(y1_o.at[:, second], yr_o.at[0], across, hl).start()
        away(dy.at[:, second], yr_o.at[1], across, hl + 1).start()

    y_in = [local(dy, st.at[0]), local(y1_o, st.at[1])]
    dk_s[...] = jnp.zeros_like(dk_s)
    dv_s[...] = jnp.zeros_like(dv_s)

    def dseen(slot, block):
        def tile(n):
            got = _nt(st[slot], wo_s[_rows(n, 4 * HEAD), :]).astype(jnp.bfloat16)
            for h in range(4):
                do_s[4 * n + h, _rows(block), :] = got[:, h * HEAD : (h + 1) * HEAD]

        _loop(0, nh // 4, tile)

    def project(slot, upper, lower):
        def tile(n):
            got = jnp.dot(st[slot], w_s[:, _rows(n, 4 * HEAD)], preferred_element_type=jnp.float32).astype(jnp.bfloat16)
            for p, place in enumerate((upper, lower)):
                rows = _rows(place, part)
                for h in range(4):
                    t = got[p * part : (p + 1) * part, h * HEAD : (h + 1) * HEAD].astype(jnp.float32)
                    t = jnp.where(n < (nq + nk) // (4 * HEAD), _turn(t, cos[rows, :], sin[rows, :]), t)
                    qkv_s[4 * n + h, rows, :] = t.astype(jnp.bfloat16)

        _loop(0, w_s.shape[1] // (4 * HEAD), tile)

    wo_in.wait()
    for slot, block in ((0, me), (1, 2 * chip + 1 - core)):
        y_in[slot].wait()
        dseen(slot, block)
    a_in = local(a0_o, st.at[0])
    for w in w_in:
        w.wait()
    a_in.wait()
    project(0, 2 * me, 2 * me + 1)
    for c in near_a:
        c.wait_recv()
    local(a1_o, st.at[1]).wait()
    other = 2 * chip + 1 - core
    project(1, 2 * other, 2 * other + 1)

    def query(i, b):
        return qkv_s[pl.ds(2 * i, 2), _rows(b), :].reshape(cols, HEAD)

    def look(b, slot, start, stop, diagonal):
        qs = [query(i, b) for i in range(kv)]

        def block(j, masked):
            scores = [_nt(qkv_s[nh + i, _rows(j), :], qs[i]) for i in range(kv)]
            for i, s in enumerate(scores):
                at = slot * kv + i
                if masked:
                    s = jnp.where(_causal(), s, 2 * NEG)
                old = top_s[at]
                top = jnp.maximum(old, s.max(axis=0, keepdims=True))
                top_s[at] = top
                p = jnp.exp2((s - top) * e).astype(jnp.bfloat16)
                values = jnp.concatenate([qkv_s[nh + kv + i, _rows(j), :].T, jnp.ones((8, BLOCK), jnp.bfloat16)], axis=0)
                mix_s[at] = mix_s[at] * jnp.exp2((old - top) * e) + _dot(values, p, 1, 0)

        _loop(start, stop, lambda j: block(j, False))
        if diagonal:
            block(b, True)

    def begin():
        top_s[...] = jnp.full_like(top_s, NEG)
        mix_s[...] = jnp.zeros_like(mix_s)

    def end(b, slot):
        for i in range(kv):
            at = slot * kv + i
            total = mix_s[at, HEAD : HEAD + 1]
            got = (mix_s[at, :HEAD] * (1 / total)).T.astype(jnp.bfloat16)
            for h in range(2):
                o_s[2 * i + h, _rows(b), :] = got[h * BLOCK : (h + 1) * BLOCK]
            lse_s[kv * b + i] = (top_s[at] * scale + jnp.log(total)) * LOG2E

    def near(b):
        look(2 * chip + b, b, 2 * chip, 2 * chip + b, True)

    def rest(b):
        look(2 * chip + b, b, 0, 2 * chip, False)
        end(2 * chip + b, b)

    def distant(b):
        look(2 * far + b, b, 0, 2 * far + b, True)
        end(2 * far + b, b)

    begin()
    _loop(0, 2, near)

    for j in range(2):
        far_a[j].wait_recv()
        onward = remote(a2_o.at[parts[j]], a3_o.at[parts[j]], beside)
        mine = local(a2_o.at[parts[j]], st.at[j, parts[0]])
        onward.wait_recv()
        local(a3_o.at[parts[j]], st.at[j, parts[1]]).wait()
        mine.wait()
        project(j, 2 * (2 * far + core) + j, 2 * (2 * far + 1 - core) + j)
        onward.wait_send()
    _loop(0, 2, rest)
    begin()
    _loop(0, 2, distant)
    seen_out = local(o_s, seen_o)

    def backward(b):
        def pair(g):
            dq_s[...] = jnp.zeros_like(dq_s)
            qs = [query(2 * g + i, b) for i in range(2)]
            dos = [do_s[pl.ds(4 * g + 2 * i, 2), _rows(b), :].reshape(cols, HEAD) for i in range(2)]
            outs = [o_s[pl.ds(4 * g + 2 * i, 2), _rows(b), :].reshape(cols, HEAD) for i in range(2)]
            deltas = [(y.astype(jnp.float32) * o.astype(jnp.float32)).T.sum(0, keepdims=True) for y, o in zip(dos, outs)]

            def block(j, masked):
                scores = [_nt(qkv_s[nh + 2 * g + i, _rows(j), :], qs[i]) for i in range(2)]
                dps = [_nt(qkv_s[nh + kv + 2 * g + i, _rows(j), :], dos[i]) for i in range(2)]
                for i in range(2):
                    at = 2 * g + i
                    p = jnp.exp2(scores[i] * e - lse_s[kv * b + at])
                    if masked:
                        p = jnp.where(_causal(), p, 0.0)
                    ds = (p * (dps[i] - deltas[i])).astype(jnp.bfloat16)
                    dv_s[at, _rows(j), :] += _dot(p.astype(jnp.bfloat16), dos[i], 1, 0)
                    dk_s[at, _rows(j), :] += _dot(ds, qs[i], 1, 0)
                    dq_s[i] += _dot(qkv_s[nh + at, _rows(j), :].T, ds, 1, 0)

            _loop(0, b, lambda j: block(j, False))
            block(b, True)
            for i in range(2):
                got = (dq_s[i] * scale).T
                for h in range(2):
                    t = got[h * BLOCK : (h + 1) * BLOCK].astype(jnp.bfloat16).astype(jnp.float32)
                    t = _unturn(t, cos[_rows(b), :], sin[_rows(b), :])
                    dqkv_s[:, _rows(4 * g + 2 * i + h, HEAD)] = t.astype(jnp.bfloat16)

        _loop(0, kv // 2, pair)

    loop_sems = used[0]
    used[0] += 8

    def loose(src, dst, at):
        return pltpu.make_async_copy(src, dst, lsem.at[loop_sems + at])

    queries = pl.ds(0, nq)

    def own(i):
        backward(2 * chip + i)
        copy = loose(dqkv_s.at[:, queries], dq_o.at[i], 0)
        copy.start()
        copy.wait()

    _loop(0, 2, own)

    def remote_block(i):
        b = 2 * far + 1 - i
        mine, others = _rows(1 - core, half), _rows(core, half)
        away(dy.at[:, first], yr_o.at[i], across, hl + i).wait_recv()
        onward = away(yr_o.at[i], yf_o.at[i], beside, on + i)
        onward.start()
        here, there = loose(yr_o.at[i], st.at[i, :, mine], 1), loose(yf_o.at[i], st.at[i, :, others], 2)
        here.start()
        onward.wait_recv()
        there.start()
        here.wait()
        there.wait()
        dseen(i, b)
        backward(b)
        q_out = loose(dqkv_s.at[:, queries], dq_o.at[2 + i], 3)
        q_out.start()
        for n in range(kv):
            t = _unturn((dk_s[n, _rows(b), :] * scale).astype(jnp.bfloat16).astype(jnp.float32), cos[_rows(b), :], sin[_rows(b), :])
            dqkv_s[:, nq + n * HEAD : nq + (n + 1) * HEAD] = t.astype(jnp.bfloat16)
            dqkv_s[:, nq + nk + n * HEAD : nq + nk + (n + 1) * HEAD] = dv_s[n, _rows(b), :].astype(jnp.bfloat16)
        kv_out = loose(dqkv_s.at[:, pl.ds(nq, 2 * nk)], dkv_o.at[i], 4)
        kv_out.start()

        steps = half // WIDE

        def term(n, side):
            return _nt(dqkv_s[...], w_s[_rows(side * steps + n, WIDE), :])

        def give(n):
            give_s[:, _rows(n, WIDE)] = term(n, core).astype(jnp.bfloat16)

        def keep(n):
            keep_s[:, _rows(n, WIDE)] = term(n, 1 - core)

        _loop(0, steps, give)
        sent = away(give_s, got_s.at[i], beside, gv + i)
        sent.start()
        _loop(0, steps, keep)
        sent.wait_recv()

        def add(n):
            rows = _rows(n, 16)
            got_s[i, rows, :] = (keep_s[rows, :] + got_s[i, rows, :].astype(jnp.float32)).astype(jnp.bfloat16)

        _loop(0, BLOCK // 16, add)
        out = [loose(got_s.at[i], o, 5) for o in (sumh_o, suml_o)]

        @pl.when(i == 0)
        def _():
            out[0].start()

        @pl.when(i == 1)
        def _():
            out[1].start()

        out[0].wait()
        sent.wait_send()
        onward.wait_send()
        q_out.wait()
        kv_out.wait()

    _loop(0, 2, remote_block)
    last = [local(dk_s, dk_o), local(dv_s, dv_o), seen_out]
    for c in last:
        c.wait()
    for c in (y1, *far_a, *near_a):
        c.wait_send()
    for i in range(2):
        away(dy.at[:, first], yr_o.at[i], across, hl + i).wait_send()


def to_gradients(x, dy, gain, wq, wk, wv, wo, cos, sin):
    _, d = x.shape
    nq, nk = wq.shape[1], wk.shape[1]
    nh, kv = nq // HEAD, nk // HEAD
    tokens = 4 * BLOCK
    f32, low = jnp.float32, jnp.bfloat16
    whole, halves = _sds((BLOCK, d)), _sds((2, BLOCK, d // 2))
    vmem = pl.BlockSpec(memory_space=pltpu.VMEM)
    shapes = [whole] * 5 + [halves] * 2 + [
        _sds((nh, tokens, HEAD)), _sds((4, BLOCK, nq)), _sds((2, BLOCK, 2 * nk)), _sds((kv, tokens, HEAD), f32),
        _sds((kv, tokens, HEAD), f32), _sds((BLOCK, d // 2)), _sds((BLOCK, d // 2))]
    return pl.pallas_call(
        _main_kernel,
        in_specs=[vmem] * 3 + [ANY] * 6,
        out_specs=[ANY] * len(shapes),
        out_shape=shapes,
        scratch_shapes=[
            pltpu.VMEM((d, nq + 2 * nk), low), pltpu.VMEM((nq, d), low), pltpu.VMEM((2, BLOCK, d), low),
            pltpu.VMEM((nh + 2 * kv, tokens, HEAD), low), pltpu.VMEM((nh, tokens, HEAD), low), pltpu.VMEM((nh, tokens, HEAD), low),
            pltpu.VMEM((4 * kv, 1, 2 * BLOCK), f32), pltpu.VMEM((2 * kv, 1, 2 * BLOCK), f32),
            pltpu.VMEM((2 * kv, HEAD + 8, 2 * BLOCK), f32), pltpu.VMEM((2, HEAD, 2 * BLOCK), f32), pltpu.VMEM((kv, tokens, HEAD), f32),
            pltpu.VMEM((kv, tokens, HEAD), f32), pltpu.VMEM((BLOCK, nq + 2 * nk), low), pltpu.VMEM((BLOCK, d // 2), low),
            pltpu.VMEM((2, BLOCK, d // 2), low), pltpu.VMEM((BLOCK, d // 2), f32),
            pltpu.SemaphoreType.DMA((32,)), pltpu.SemaphoreType.DMA((16,)), pltpu.SemaphoreType.DMA((16,))],
        compiler_params=pltpu.CompilerParams(vmem_limit_bytes=VMEM, collective_id=0, has_side_effects=True),
        cost_estimate=_estimate(2 * tokens * d * (3 * nq + 2 * nk), wq, wk, wv, wo),
    )(gain, cos, sin, x, dy, wq, wk, wv, wo)


WIDE = 768


def _dkv(dk_ref, dv_ref, cos_ref, sin_ref):
    scale = HEAD**-0.5
    parts = [_unturn((dk_ref[i] * scale).astype(jnp.bfloat16).astype(jnp.float32), cos_ref[...], sin_ref[...]).astype(jnp.bfloat16)
             for i in range(dk_ref.shape[0])]
    parts += [dv_ref[i].astype(jnp.bfloat16) for i in range(dv_ref.shape[0])]
    return jnp.concatenate(parts, axis=1)


def _term(dq, dkv, wq, wk, wv):
    half = dkv.shape[1] // 2
    return _nt(dq, wq[...]) + _nt(dkv[:, :half], wk[...]) + _nt(dkv[:, half:], wv[...])


def _weight_tiles(wq, wk, wv, tile):
    return [pl.BlockSpec((WIDE, w.shape[1]), lambda n, ids: (tile(n, ids), 0)) for w in (wq, wk, wv)]


def _own_kernel(ids, dq_ref, dk_ref, dv_ref, cos_ref, sin_ref, wq, wk, wv, mine_ref, other_ref, dkv_ref):
    @pl.when(pl.program_id(0) == 0)
    def _():
        dkv_ref[...] = _dkv(dk_ref, dv_ref, cos_ref, sin_ref)

    for out_ref, place in ((mine_ref, ids[1]), (other_ref, 1 - ids[1])):
        rows = pl.ds(pl.multiple_of(place * BLOCK, BLOCK), BLOCK)
        out_ref[...] = _term(dq_ref[rows, :], dkv_ref[rows, :], wq, wk, wv).astype(out_ref.dtype)


def own_terms(ids, dq, dk, dv, cos, sin, wq, wk, wv):
    d = wq.shape[0]
    width = dq.shape[1]
    keys = pl.BlockSpec((dk.shape[0], 2 * BLOCK, HEAD), lambda n, ids: (0, ids[2], 0))
    table = pl.BlockSpec((2 * BLOCK, HEAD), lambda n, ids: (ids[2], 0))
    whole = pl.BlockSpec((2 * BLOCK, width), lambda n, ids: (0, 0))
    part = pl.BlockSpec((BLOCK, WIDE), lambda n, ids: (0, n))
    return pl.pallas_call(
        _own_kernel,
        grid_spec=pltpu.PrefetchScalarGridSpec(
            num_scalar_prefetch=1,
            grid=(d // WIDE,),
            in_specs=[whole, keys, keys, table, table, *_weight_tiles(wq, wk, wv, lambda n, ids: n)],
            out_specs=[part, part, whole],
        ),
        out_shape=[_sds((BLOCK, d), jnp.float32), _sds((BLOCK, d)), _sds((2 * BLOCK, width))],
        compiler_params=_params("arbitrary"),
        cost_estimate=_estimate(8 * BLOCK * d * width, wq, wk, wv),
    )(ids, dq, dk, dv, cos, sin, wq, wk, wv)


def _dw_kernel(ids, a0, a1, a2, a3, q, e, f, oq, ok, ov, all_s):
    core = ids[1]
    half = q.shape[1]

    @pl.when(pl.program_id(0) == 0)
    def _():
        for i, slot in enumerate((core, 1 - core, 3 - core, 2 + core)):
            rows = _rows(slot)
            all_s[rows, :half] = q[i * BLOCK : (i + 1) * BLOCK, :]
            all_s[rows, half:] = (e if i < 2 else f)[i % 2 * BLOCK : (i % 2 + 1) * BLOCK, :]

    a = jnp.concatenate([a0[...], a1[...], a2[...], a3[...]], axis=0)
    at = a.T
    nq, nk = oq.shape[1], ok.shape[1]
    for first, out_ref in ((0, oq), (nq, ok), (nq + nk, ov)):
        out_ref[...] = jnp.dot(at, all_s[:, first : first + out_ref.shape[1]], preferred_element_type=jnp.float32).astype(jnp.bfloat16)


def weight_grads(ids, states, dq, dkvs, nk):
    d = states[0].shape[1]
    nq = dq.shape[1]
    wide = 512
    whole = lambda a: pl.BlockSpec(a.shape, lambda n, ids: (0, 0))
    outs = (nq, nk, nk)
    return pl.pallas_call(
        _dw_kernel,
        grid_spec=pltpu.PrefetchScalarGridSpec(
            num_scalar_prefetch=1,
            grid=(d // wide,),
            in_specs=[*[pl.BlockSpec((BLOCK, wide), lambda n, ids: (0, n)) for _ in states], *[whole(a) for a in (dq, *dkvs)]],
            out_specs=[pl.BlockSpec((wide, n), lambda i, ids: (i, 0)) for n in outs],
            scratch_shapes=[pltpu.VMEM((4 * BLOCK, nq + 2 * nk), jnp.bfloat16)],
        ),
        out_shape=[_sds((d, n)) for n in outs],
        compiler_params=_params("arbitrary"),
        cost_estimate=_estimate(8 * BLOCK * d * (nq + 2 * nk), *states, dq, *dkvs),
    )(ids, *states, dq, *dkvs)


def _dwo_kernel(ids, seen, y0, y1, yr, yf, out_ref, t_s):
    core = ids[1]
    n = pl.program_id(0)

    @pl.when(n == 0)
    def _():
        blocks = (ids[0], 2 * ids[2] + 1 - core, ids[4], ids[5])
        for h in range(seen.shape[0]):
            rows = jnp.concatenate([seen[h, _rows(i), :] for i in blocks], axis=0)
            t_s[h * HEAD : (h + 1) * HEAD, :] = rows.T

    first = n < pl.num_programs(0) // 2
    far = jnp.where(first, yr[...], yf[...])
    y = jnp.concatenate([y0[...], y1[...], far[0], far[1]], axis=0)
    out_ref[...] = jnp.dot(t_s[...], y, preferred_element_type=jnp.float32).astype(jnp.bfloat16)


def wo_grad(ids, seen, y0, y1, yr, yf):
    d = y0.shape[1]
    steps = d // WIDE
    half = steps // 2
    rows = seen.shape[0] * HEAD

    def at(n, ids):
        return 0, lax.rem(n + (1 - ids[1]) * half, steps)

    r = pl.BlockSpec((2, BLOCK, WIDE), lambda n, ids: (0, 0, jnp.minimum(n, half - 1)))
    f = pl.BlockSpec((2, BLOCK, WIDE), lambda n, ids: (0, 0, jnp.maximum(n - half, 0)))
    whole = pl.BlockSpec(seen.shape, lambda n, ids: (0, 0, 0))
    y = pl.BlockSpec((BLOCK, WIDE), at)
    return pl.pallas_call(
        _dwo_kernel,
        grid_spec=pltpu.PrefetchScalarGridSpec(
            num_scalar_prefetch=1,
            grid=(steps,),
            in_specs=[whole, y, y, r, f],
            out_specs=pl.BlockSpec((rows, WIDE), at),
            scratch_shapes=[pltpu.VMEM((rows, 4 * BLOCK), jnp.bfloat16)],
        ),
        out_shape=_sds((rows, d)),
        compiler_params=_params("arbitrary"),
        cost_estimate=_estimate(8 * BLOCK * d * rows, seen, y0, y1, yr, yf),
    )(ids, seen, y0, y1, yr, yf)


def _finish_kernel(ids, x_ref, dy_ref, gain_ref, mine_ref, other_ref, rh, rl, fh, fl, dx_ref, dgain_ref):
    upper = ids[1] == 1
    left = jnp.where(upper, rh[...], fl[...])
    right = jnp.where(upper, fh[...], rl[...])
    da = mine_ref[...] + other_ref[...].astype(jnp.float32) + jnp.concatenate([left, right], axis=1).astype(jnp.float32)
    x = x_ref[...].astype(jnp.float32)
    scale = lax.rsqrt(jnp.mean(x * x, -1, keepdims=True) + 1e-6)
    hat = x * scale
    by_hat = da * gain_ref[...].astype(jnp.float32)
    dx = scale * (by_hat - hat * jnp.mean(by_hat * hat, -1, keepdims=True))
    dx_ref[...] = (dy_ref[...].astype(jnp.float32) + dx).astype(jnp.bfloat16)
    part = (da * hat).sum(0, keepdims=True)

    @pl.when(pl.program_id(0) == 0)
    def _():
        dgain_ref[...] = part

    @pl.when(pl.program_id(0) > 0)
    def _():
        dgain_ref[...] += part


def finish(ids, x, dy, gain, mine, other, rh, rl, fh, fl):
    rows, d = x.shape
    step = 64
    whole = pl.BlockSpec((step, d), lambda i, ids: (i, 0))
    half = pl.BlockSpec((step, d // 2), lambda i, ids: (i, 0))
    one = pl.BlockSpec((1, d), lambda i, ids: (0, 0))
    return pl.pallas_call(
        _finish_kernel,
        grid_spec=pltpu.PrefetchScalarGridSpec(
            num_scalar_prefetch=1,
            grid=(rows // step,),
            in_specs=[whole, whole, one, whole, whole, half, half, half, half],
            out_specs=[whole, one],
        ),
        out_shape=[_sds((rows, d)), _sds((1, d), jnp.float32)],
        compiler_params=_params("arbitrary"),
        cost_estimate=_estimate(20 * x.size, x, dy, mine, other),
    )(ids, x, dy, gain, mine, other, rh, rl, fh, fl)


def solution(mesh):
    across = [(i, i ^ 2) for i in range(4)]
    beside = [(i, i ^ 1) for i in range(4)]
    up = [(0, 1), (2, 3)]
    down = [(1, 0), (3, 2)]

    def send(a, pairs):
        return lax.ppermute(a, "tp", pairs)

    def body(x, dy, gain, wq, wk, wv, wo):
        gain = gain[None]
        me = lax.axis_index("tp").astype(jnp.int32)
        core, chip = me % 2, me // 2
        ids = jnp.stack([me, core, chip, 1 - chip, 2 * (1 - chip) + 1, 2 * (1 - chip)])
        half = HEAD // 2
        angle = jnp.arange(4 * BLOCK).astype(jnp.float32)[:, None] * THETA ** (-jnp.arange(half, dtype=jnp.float32) / half)
        cos, sin = jnp.cos(angle), jnp.sin(angle)
        cos, sin = jnp.concatenate([cos, cos], 1), jnp.concatenate([-sin, sin], 1)

        a0, a1, a2, a3, y1, yr, yf, seen, dq, dkv_far, dk, dv, sum_h, sum_l = to_gradients(
            x, dy, gain, wq, wk, wv, wo, cos, sin)
        rh, rl = send(sum_h, across), send(sum_l, across)
        fh, fl = send(rh, up), send(rl, down)
        dq, dkv_far = dq.reshape(4 * BLOCK, -1), dkv_far.reshape(2 * BLOCK, -1)
        mine, other, dkv_own = own_terms(ids, dq, dk, dv, cos, sin, wq, wk, wv)
        other = send(other, beside)
        dwo = wo_grad(ids, seen, dy, y1, yr, yf)
        dwq, dwk, dwv = weight_grads(ids, (a0, a1, a2, a3), dq, (dkv_own, dkv_far), wk.shape[1])
        dx, dgain = finish(ids, x, dy, gain, mine, other, rh, rl, fh, fl)
        dgain = dgain + send(dgain, beside)
        dgain = dgain + send(dgain, across)
        return dx, dgain, dwq, dwk, dwv, dwo

    tokens, columns = P(("dp", "tp"), None), P(None, "tp")
    return jax.shard_map(
        body,
        mesh=mesh,
        in_specs=(tokens, tokens, P(None), columns, columns, columns, P("tp", None)),
        out_specs=(tokens, P("dp", None), P("dp", "tp"), P("dp", "tp"), P("dp", "tp"), P(("dp", "tp"), None)),
        check_vma=False,
    )
```

```python
import jax
import jax.numpy as jnp
import numpy as np
from jax import lax
from jax.experimental import pallas as pl
from jax.experimental.pallas import tpu as pltpu

from jax.sharding import PartitionSpec as P

NEG = -1e30
LOG2E = 1.4426950408889634
VMEM = 67043328
HEAD = 128
THETA = 10000
BLOCK = 256


def _params(*semantics):
    return pltpu.CompilerParams(dimension_semantics=semantics, vmem_limit_bytes=VMEM)


def _estimate(flops, *arrays):
    return pl.CostEstimate(flops=flops, transcendentals=0, bytes_accessed=sum(a.size * a.dtype.itemsize for a in arrays))


def _sds(shape, dtype=jnp.bfloat16):
    return jax.ShapeDtypeStruct(shape, dtype)


ANY = pl.BlockSpec(memory_space=pl.ANY)


def _dot(a, b, ca, cb):
    return lax.dot_general(a, b, (((ca,), (cb,)), ((), ())), preferred_element_type=jnp.float32)


def _nt(a, b):
    return _dot(a, b, 1, 1)


def _turn(t, table, back=False):
    swapped = pltpu.roll(table, HEAD // 2, 1)
    low = lax.broadcasted_iota(jnp.int32, table.shape, 1) < HEAD // 2
    cos, sin = jnp.where(low, table, swapped), jnp.where(low, -swapped, table)
    turn = pltpu.roll(t, HEAD // 2, 1) * sin
    return t * cos - turn if back else t * cos + turn


def _causal():
    shape = (BLOCK, 2 * BLOCK)
    return lax.rem(lax.broadcasted_iota(jnp.int32, shape, 1), BLOCK) >= lax.broadcasted_iota(jnp.int32, shape, 0)


def _rows(block, size=BLOCK):
    return pl.ds(pl.multiple_of(block * size, size), size)


def _loop(first, last, body):
    lax.fori_loop(first, last, lambda i, _: body(i), None)


def _main_kernel(gain, table, x, dy, wq, wk, wv, wo,
                 a0_o, a1_o, a2_o, a3_o, y1_o, yr_o, yf_o, seen_o, dq_o, dkv_o, sumh_o, suml_o, far_o, mine_o, other_o,
                 w_s, wo_s, st, qkv_s, do_s, o_s, lse_s, top_s, mix_s, dq_s, dk_s, dv_s, dqkv_s, give_s, got_s, keep_s,
                 lsem, ssem, rsem):
    dp, me = lax.axis_index("dp"), lax.axis_index("tp")
    core, chip = lax.rem(me, 2), lax.div(me, 2)
    beside, across = (dp, me + 1 - 2 * core), (dp, lax.rem(me + 2, 4))
    far = 1 - chip
    d = x.shape[1]
    half, part = d // 2, BLOCK // 2
    scale = HEAD**-0.5
    e = scale * LOG2E
    cols = 2 * BLOCK
    nh, kv = do_s.shape[0], dk_s.shape[0]
    MESH = pl.DeviceIdType.MESH

    barrier = pltpu.get_barrier_semaphore()
    for peer in range(1, 4):
        pl.semaphore_signal(barrier, inc=1, device_id=(dp, lax.rem(me + peer, 4)), device_id_type=MESH)
    pl.semaphore_wait(barrier, 3)

    used = [0, 0]

    def local(src, dst):
        copy = pltpu.make_async_copy(src, dst, lsem.at[used[0]])
        used[0] += 1
        copy.start()
        return copy

    def away(src, dst, to, at):
        return pltpu.make_async_remote_copy(src_ref=src, dst_ref=dst, send_sem=ssem.at[at], recv_sem=rsem.at[at], device_id=to,
                                            device_id_type=MESH)

    def remote(src, dst, to):
        copy = away(src, dst, to, used[1])
        used[1] += 1
        copy.start()
        return copy

    parts = [pl.ds(j * part, part) for j in range(2)]
    y1 = remote(dy, y1_o, beside)
    xs = [local(x.at[r], st.at[0, r]) for r in parts]
    nq, nk = wq.shape[1], wk.shape[1]
    wo_in = local(wo, wo_s)
    w_in = [local(w, w_s.at[:, pl.ds(at, w.shape[1])]) for w, at in ((wq, 0), (wk, nq), (wv, nq + nk))]
    far_a, near_a = [], []
    for j in range(2):
        xs[j].wait()

        def norm(i):
            rows = pl.ds(pl.multiple_of(j * part + i * 16, 16), 16)
            wide = st[0, rows, :].astype(jnp.float32)
            inv = lax.rsqrt(jnp.mean(wide * wide, -1, keepdims=True) + 1e-6)
            st[1, rows, :] = (wide * inv * gain[...].astype(jnp.float32)[None, :]).astype(jnp.bfloat16)

        _loop(0, part // 16, norm)
        local(st.at[1, parts[j]], a0_o.at[parts[j]]).wait()
        far_a.append(remote(a0_o.at[parts[j]], a2_o.at[parts[j]], across))
        near_a.append(remote(a0_o.at[parts[j]], a1_o.at[parts[j]], beside))

    y1.wait_recv()
    first, second = pl.ds(0, half), pl.ds(half, half)
    hl = used[1]
    on = hl + 2
    gv = hl + 4
    across_h = hl + 6
    own_other = hl + 8
    used[1] += 8 + d // WIDE

    @pl.when(core == 1)
    def _():
        away(dy.at[:, first], yr_o.at[0], across, hl).start()
        away(y1_o.at[:, first], yr_o.at[1], across, hl + 1).start()

    @pl.when(core == 0)
    def _():
        away(y1_o.at[:, second], yr_o.at[0], across, hl).start()
        away(dy.at[:, second], yr_o.at[1], across, hl + 1).start()

    y_in = [local(dy, st.at[0]), local(y1_o, st.at[1])]
    dk_s[...] = jnp.zeros_like(dk_s)
    dv_s[...] = jnp.zeros_like(dv_s)

    def dseen(slot, block):
        def tile(n):
            got = _nt(st[slot], wo_s[_rows(n, 4 * HEAD), :]).astype(jnp.bfloat16)
            for h in range(4):
                do_s[4 * n + h, _rows(block), :] = got[:, h * HEAD : (h + 1) * HEAD]

        _loop(0, nh // 4, tile)

    def project(slot, upper, lower):
        def tile(n):
            got = jnp.dot(st[slot], w_s[:, _rows(n, 4 * HEAD)], preferred_element_type=jnp.float32).astype(jnp.bfloat16)
            for p, place in enumerate((upper, lower)):
                rows = _rows(place, part)
                for h in range(4):
                    t = got[p * part : (p + 1) * part, h * HEAD : (h + 1) * HEAD].astype(jnp.float32)
                    t = jnp.where(n < (nq + nk) // (4 * HEAD), _turn(t, table[rows, :]), t)
                    qkv_s[4 * n + h, rows, :] = t.astype(jnp.bfloat16)

        _loop(0, w_s.shape[1] // (4 * HEAD), tile)

    wo_in.wait()
    for slot, block in ((0, me), (1, 2 * chip + 1 - core)):
        y_in[slot].wait()
        dseen(slot, block)
    a_in = local(a0_o, st.at[0])
    for w in w_in:
        w.wait()
    a_in.wait()
    project(0, 2 * me, 2 * me + 1)
    for c in near_a:
        c.wait_recv()
    local(a1_o, st.at[1]).wait()
    other = 2 * chip + 1 - core
    project(1, 2 * other, 2 * other + 1)

    def query(i, b):
        return qkv_s[pl.ds(2 * i, 2), _rows(b), :].reshape(cols, HEAD)

    def look(b, slot, start, stop, diagonal):
        qs = [query(i, b) for i in range(kv)]

        def block(j, masked):
            scores = [_nt(qkv_s[nh + i, _rows(j), :], qs[i]) for i in range(kv)]
            for i, s in enumerate(scores):
                at = slot * kv + i
                if masked:
                    s = jnp.where(_causal(), s, 2 * NEG)
                old = top_s[at]
                top = jnp.maximum(old, s.max(axis=0, keepdims=True))
                top_s[at] = top
                p = jnp.exp2((s - top) * e).astype(jnp.bfloat16)
                values = jnp.concatenate([qkv_s[nh + kv + i, _rows(j), :].T, jnp.ones((8, BLOCK), jnp.bfloat16)], axis=0)
                mix_s[at] = mix_s[at] * jnp.exp2((old - top) * e) + _dot(values, p, 1, 0)

        _loop(start, stop, lambda j: block(j, False))
        if diagonal:
            block(b, True)

    def begin():
        top_s[...] = jnp.full_like(top_s, NEG)
        mix_s[...] = jnp.zeros_like(mix_s)

    def end(b, slot):
        for i in range(kv):
            at = slot * kv + i
            total = mix_s[at, HEAD : HEAD + 1]
            got = (mix_s[at, :HEAD] * (1 / total)).T.astype(jnp.bfloat16)
            for h in range(2):
                o_s[2 * i + h, _rows(b), :] = got[h * BLOCK : (h + 1) * BLOCK]
            lse_s[kv * b + i] = (top_s[at] * scale + jnp.log(total)) * LOG2E

    def near(b):
        look(2 * chip + b, b, 2 * chip, 2 * chip + b, True)

    def rest(b):
        look(2 * chip + b, b, 0, 2 * chip, False)
        end(2 * chip + b, b)

    def distant(b):
        look(2 * far + b, b, 0, 2 * far + b, True)
        end(2 * far + b, b)

    begin()
    _loop(0, 2, near)

    for j in range(2):
        far_a[j].wait_recv()
        onward = remote(a2_o.at[parts[j]], a3_o.at[parts[j]], beside)
        mine = local(a2_o.at[parts[j]], st.at[j, parts[0]])
        onward.wait_recv()
        local(a3_o.at[parts[j]], st.at[j, parts[1]]).wait()
        mine.wait()
        project(j, 2 * (2 * far + core) + j, 2 * (2 * far + 1 - core) + j)
        onward.wait_send()
    _loop(0, 2, rest)
    begin()
    _loop(0, 2, distant)
    seen_out = local(o_s, seen_o)

    def backward(b):
        def pair(g):
            dq_s[...] = jnp.zeros_like(dq_s)
            qs = [query(2 * g + i, b) for i in range(2)]
            dos = [do_s[pl.ds(4 * g + 2 * i, 2), _rows(b), :].reshape(cols, HEAD) for i in range(2)]
            outs = [o_s[pl.ds(4 * g + 2 * i, 2), _rows(b), :].reshape(cols, HEAD) for i in range(2)]
            deltas = [(y.astype(jnp.float32) * o.astype(jnp.float32)).T.sum(0, keepdims=True) for y, o in zip(dos, outs)]

            def block(j, masked):
                scores = [_nt(qkv_s[nh + 2 * g + i, _rows(j), :], qs[i]) for i in range(2)]
                dps = [_nt(qkv_s[nh + kv + 2 * g + i, _rows(j), :], dos[i]) for i in range(2)]
                for i in range(2):
                    at = 2 * g + i
                    p = jnp.exp2(scores[i] * e - lse_s[kv * b + at])
                    if masked:
                        p = jnp.where(_causal(), p, 0.0)
                    ds = (p * (dps[i] - deltas[i])).astype(jnp.bfloat16)
                    dv_s[at, _rows(j), :] += _dot(p.astype(jnp.bfloat16), dos[i], 1, 0)
                    dk_s[at, _rows(j), :] += _dot(ds, qs[i], 1, 0)
                    dq_s[i] += _dot(qkv_s[nh + at, _rows(j), :].T, ds, 1, 0)

            _loop(0, b, lambda j: block(j, False))
            block(b, True)
            for i in range(2):
                got = (dq_s[i] * scale).T
                for h in range(2):
                    t = got[h * BLOCK : (h + 1) * BLOCK].astype(jnp.bfloat16).astype(jnp.float32)
                    t = _turn(t, table[_rows(b), :], True)
                    dqkv_s[:, _rows(4 * g + 2 * i + h, HEAD)] = t.astype(jnp.bfloat16)

        _loop(0, kv // 2, pair)

    loop_sems = used[0]
    used[0] += 8 + d // WIDE

    def loose(src, dst, at):
        return pltpu.make_async_copy(src, dst, lsem.at[loop_sems + at])

    queries = pl.ds(0, nq)

    def own(i):
        backward(2 * chip + i)
        copy = loose(dqkv_s.at[:, queries], dq_o.at[i], 0)
        copy.start()
        copy.wait()

    _loop(0, 2, own)

    def sum_away(side):
        return away(sumh_o, far_o.at[:, _rows(1 - side, half)], (dp, 2 * far + 1), across_h + side)

    def turn_back(b, at):
        for n in range(kv):
            t = _turn((dk_s[n, _rows(b), :] * scale).astype(jnp.bfloat16).astype(jnp.float32), table[_rows(b), :], True)
            dqkv_s[:, nq + n * HEAD : nq + (n + 1) * HEAD] = t.astype(jnp.bfloat16)
            dqkv_s[:, nq + nk + n * HEAD : nq + nk + (n + 1) * HEAD] = dv_s[n, _rows(b), :].astype(jnp.bfloat16)
        copy = loose(dqkv_s.at[:, pl.ds(nq, 2 * nk)], dkv_o.at[at], 4)
        copy.start()
        return copy

    def term(n):
        return _nt(dqkv_s[...], w_s[_rows(n, WIDE), :])

    def remote_block(i):
        b = 2 * far + 1 - i
        mine, others = _rows(1 - core, half), _rows(core, half)
        away(dy.at[:, first], yr_o.at[i], across, hl + i).wait_recv()
        onward = away(yr_o.at[i], yf_o.at[i], beside, on + i)
        onward.start()
        here, there = loose(yr_o.at[i], st.at[i, :, mine], 1), loose(yf_o.at[i], st.at[i, :, others], 2)
        here.start()
        onward.wait_recv()
        there.start()
        here.wait()
        there.wait()
        dseen(i, b)
        backward(b)
        q_out = loose(dqkv_s.at[:, queries], dq_o.at[2 + i], 3)
        q_out.start()
        kv_out = turn_back(b, 2 + i)

        steps = half // WIDE

        def give(n):
            give_s[:, _rows(n, WIDE)] = term(core * steps + n).astype(jnp.bfloat16)

        def keep(n):
            keep_s[:, _rows(n, WIDE)] = term((1 - core) * steps + n)

        _loop(0, steps, give)
        sent = away(give_s, got_s.at[i], beside, gv + i)
        sent.start()
        _loop(0, steps, keep)
        sent.wait_recv()

        def add(n):
            rows = _rows(n, 16)
            got_s[i, rows, :] = (keep_s[rows, :] + got_s[i, rows, :].astype(jnp.float32)).astype(jnp.bfloat16)

        _loop(0, BLOCK // 16, add)
        out = [loose(got_s.at[i], o, 5) for o in (sumh_o, suml_o)]

        @pl.when(i == 0)
        def _():
            out[0].start()

        @pl.when(i == 1)
        def _():
            out[1].start()

        out[0].wait()

        @pl.when(i == 0)
        def _():
            sum_away(core).start()

        sent.wait_send()
        onward.wait_send()
        q_out.wait()
        kv_out.wait()

    _loop(0, 2, remote_block)
    tiles = d // WIDE
    slots = half // WIDE

    def gather_own(place):
        load = loose(dq_o.at[place], dqkv_s.at[:, queries], 0)
        load.start()
        out = turn_back(2 * chip + place, place)
        load.wait()
        return out

    def other_out(n):
        return away(give_s.at[:, _rows(lax.rem(n, slots), WIDE)], other_o.at[:, _rows(n, WIDE)], beside, own_other + n)

    def mine_out(n):
        return pltpu.make_async_copy(keep_s.at[:, _rows(lax.rem(n, slots), WIDE)], mine_o.at[:, _rows(n, WIDE)], lsem.at[loop_sems + 8 + n])

    def other_tile(n):
        @pl.when(n >= slots)
        def _():
            other_out(n - slots).wait_send()

        give_s[:, _rows(lax.rem(n, slots), WIDE)] = term(n).astype(jnp.bfloat16)
        other_out(n).start()

    def mine_tile(n):
        @pl.when(n >= slots)
        def _():
            mine_out(n - slots).wait()

        keep_s[:, _rows(lax.rem(n, slots), WIDE)] = term(n)
        mine_out(n).start()

    kv_out = gather_own(1 - core)
    _loop(0, tiles, other_tile)
    kv_out.wait()
    kv_out = gather_own(core)
    _loop(0, tiles, mine_tile)
    kv_out.wait()
    seen_out.wait()
    for n in range(tiles):
        other_out(n).wait_recv()
        if n >= slots:
            other_out(n).wait_send()
            mine_out(n).wait()
    for c in (y1, *far_a, *near_a):
        c.wait_send()
    for i in range(2):
        away(dy.at[:, first], yr_o.at[i], across, hl + i).wait_send()
    sum_away(core).wait_send()

    @pl.when(core == 1)
    def _():
        for side in range(2):
            sum_away(side).wait_recv()


WIDE = 768


def to_gradients(x, dy, gain, wq, wk, wv, wo, table):
    _, d = x.shape
    nq, nk = wq.shape[1], wk.shape[1]
    nh, kv = nq // HEAD, nk // HEAD
    tokens = 4 * BLOCK
    f32, low = jnp.float32, jnp.bfloat16
    whole, halves = _sds((BLOCK, d)), _sds((2, BLOCK, d // 2))
    vmem = pl.BlockSpec(memory_space=pltpu.VMEM)
    shapes = [whole] * 5 + [halves] * 2 + [
        _sds((nh, tokens, HEAD)), _sds((4, BLOCK, nq)), _sds((4, BLOCK, 2 * nk)), *[_sds((BLOCK, d // 2))] * 2,
        whole, _sds((BLOCK, d), f32), whole]
    return pl.pallas_call(
        _main_kernel,
        in_specs=[vmem] * 2 + [ANY] * 6,
        out_specs=[ANY] * len(shapes),
        out_shape=shapes,
        scratch_shapes=[
            pltpu.VMEM((d, nq + 2 * nk), low), pltpu.VMEM((nq, d), low), pltpu.VMEM((2, BLOCK, d), low),
            pltpu.VMEM((nh + 2 * kv, tokens, HEAD), low), pltpu.VMEM((nh, tokens, HEAD), low), pltpu.VMEM((nh, tokens, HEAD), low),
            pltpu.VMEM((4 * kv, 1, 2 * BLOCK), f32), pltpu.VMEM((2 * kv, 1, 2 * BLOCK), f32),
            pltpu.VMEM((2 * kv, HEAD + 8, 2 * BLOCK), f32), pltpu.VMEM((2, HEAD, 2 * BLOCK), f32), pltpu.VMEM((kv, tokens, HEAD), f32),
            pltpu.VMEM((kv, tokens, HEAD), f32), pltpu.VMEM((BLOCK, nq + 2 * nk), low), pltpu.VMEM((BLOCK, d // 2), low),
            pltpu.VMEM((2, BLOCK, d // 2), low), pltpu.VMEM((BLOCK, d // 2), f32),
            *[pltpu.SemaphoreType.DMA((40,))] * 3],
        compiler_params=pltpu.CompilerParams(vmem_limit_bytes=VMEM, collective_id=0, has_side_effects=True),
        cost_estimate=_estimate(2 * tokens * d * (4 * nq + 4 * nk), wq, wk, wv, wo),
    )(gain, table, x, dy, wq, wk, wv, wo)


def _grads_kernel(ids, seen, y0, y1, yr, yf, a0, a1, a2, a3, dq_in, dkv_in, dwo_ref, oq, ok, ov, t_s, dq_s, dkv_s, sem):
    core, n = ids[1], pl.program_id(0)
    steps = pl.num_programs(0) // 2
    loads = [pltpu.make_async_copy(a, b, sem.at[i]) for i, (a, b) in enumerate(((dq_in, dq_s), (dkv_in, dkv_s)))]

    @pl.when(n == 0)
    def _():
        for load in loads:
            load.start()
        blocks = (ids[0], 2 * ids[2] + 1 - core, ids[4], ids[5])
        for h in range(seen.shape[0]):
            rows = jnp.concatenate([seen[h, _rows(i), :] for i in blocks], axis=0)
            t_s[h * HEAD : (h + 1) * HEAD, :] = rows.T

    @pl.when(n < steps)
    def _():
        first = n < steps // 2
        far = jnp.where(first, yr[...], yf[...])
        y = jnp.concatenate([y0[...], y1[...], far[0], far[1]], axis=0)
        dwo_ref[...] = jnp.dot(t_s[...], y, preferred_element_type=jnp.float32).astype(jnp.bfloat16)

    @pl.when(n == steps)
    def _():
        for load in loads:
            load.wait()

    @pl.when(n >= steps)
    def _():
        upper = core == 1
        pick = lambda p, q: jnp.where(upper, p[...], q[...])
        a = jnp.concatenate([pick(a1, a0), pick(a0, a1), pick(a2, a3), pick(a3, a2)], axis=0)
        at = a.T
        nk = ok.shape[1]
        for grad, out_ref in ((dq_s[...], oq), (dkv_s[:, :nk], ok), (dkv_s[:, nk:], ov)):
            out_ref[...] = jnp.dot(at, grad, preferred_element_type=jnp.float32).astype(jnp.bfloat16)


def weight_grads(ids, seen, y0, y1, yr, yf, states, dq, dkv):
    d = y0.shape[1]
    steps = d // WIDE
    half = steps // 2
    nq, nk = dq.shape[1], dkv.shape[1] // 2
    outs = (nq, nk, nk)
    low = jnp.bfloat16

    def at(n, ids):
        return 0, lax.rem(jnp.minimum(n, steps - 1) + (1 - ids[1]) * half, steps)

    def later(n):
        return jnp.maximum(n - steps, 0)

    r = pl.BlockSpec((2, BLOCK, WIDE), lambda n, ids: (0, 0, jnp.minimum(n, half - 1)))
    f = pl.BlockSpec((2, BLOCK, WIDE), lambda n, ids: (0, 0, jnp.clip(n - half, 0, half - 1)))
    y = pl.BlockSpec((BLOCK, WIDE), at)
    state = pl.BlockSpec((BLOCK, WIDE), lambda n, ids: (0, later(n)))
    return pl.pallas_call(
        _grads_kernel,
        grid_spec=pltpu.PrefetchScalarGridSpec(
            num_scalar_prefetch=1,
            grid=(2 * steps,),
            in_specs=[pl.BlockSpec(seen.shape, lambda n, ids: (0, 0, 0)), y, y, r, f, *[state] * 4, ANY, ANY],
            out_specs=[pl.BlockSpec((nq, WIDE), at), *[pl.BlockSpec((WIDE, w), lambda n, ids: (later(n), 0)) for w in outs]],
            scratch_shapes=[pltpu.VMEM((nq, 4 * BLOCK), low), pltpu.VMEM(dq.shape, low), pltpu.VMEM(dkv.shape, low),
                            pltpu.SemaphoreType.DMA((2,))],
        ),
        out_shape=[_sds((nq, d)), *[_sds((d, w)) for w in outs]],
        compiler_params=_params("arbitrary"),
        cost_estimate=_estimate(8 * BLOCK * d * 2 * (nq + nk), seen, y0, y1, yr, yf, *states, dq, dkv),
    )(ids, seen, y0, y1, yr, yf, *states, dq, dkv)


def _finish_kernel(ids, gain, x, dy, mine, other, far_h, left_l, right_l, dx, dgain_ref, *rest):
    *bufs, out_s, sum_s, sem, out_sem = rest
    rows, d = x.shape
    step, half = rows // sem.shape[0], d // 2
    upper = ids[1] == 1

    def loads(c, core):
        here = pl.ds(c * step, step)
        first, second = pl.ds(0, half), pl.ds(half, half)
        given = [a.at[here] for a in (x, dy, mine, other)]
        given += [far_h.at[here, first], far_h.at[here, second]] if core else [left_l.at[here], right_l.at[here]]
        dsts = (*[b.at[here] for b in bufs[:4]], bufs[4].at[here, first], bufs[4].at[here, second])
        return [pltpu.make_async_copy(a, b, sem.at[c, n]) for n, (a, b) in enumerate(zip(given, dsts))]

    for core in range(2):
        @pl.when(upper if core else ~upper)
        def _():
            for c in range(sem.shape[0]):
                for load in loads(c, core):
                    load.start()

    sum_s[...] = jnp.zeros_like(sum_s)
    group = sum_s.shape[0]
    outs = []
    for c in range(sem.shape[0]):
        for load in loads(c, 0):
            load.wait()

        def some(i):
            at = pl.ds(pl.multiple_of(c * step + i * group, group), group)
            wide, y, m, o, f = (b[at, :].astype(jnp.float32) for b in bufs)
            da = m + o + f
            scale = lax.rsqrt(jnp.mean(wide * wide, -1, keepdims=True) + 1e-6)
            hat = wide * scale
            by_hat = da * gain[...].astype(jnp.float32)[None, :]
            sum_s[...] += da * hat
            dx_part = scale * (by_hat - hat * jnp.mean(by_hat * hat, -1, keepdims=True))
            out_s[at, :] = (y + dx_part).astype(jnp.bfloat16)

        _loop(0, step // group, some)
        here = pl.ds(c * step, step)
        outs.append(pltpu.make_async_copy(out_s.at[here], dx.at[here], out_sem.at[c]))
        outs[-1].start()
    dgain_ref[...] = sum_s[...].sum(0, keepdims=True)
    for out in outs:
        out.wait()


def finish(ids, x, dy, gain, mine, other, far_h, left_l, right_l):
    rows, d = x.shape
    chunks = 4
    low, f32 = jnp.bfloat16, jnp.float32
    smem, vmem = pl.BlockSpec(memory_space=pltpu.SMEM), pl.BlockSpec(memory_space=pltpu.VMEM)
    return pl.pallas_call(
        _finish_kernel,
        in_specs=[smem, vmem, *[ANY] * 7],
        out_specs=[ANY, vmem],
        out_shape=[_sds((rows, d)), _sds((1, d), f32)],
        scratch_shapes=[*[pltpu.VMEM((rows, d), t) for t in (low, low, f32, low, low, low)], pltpu.VMEM((32, d), f32),
                        pltpu.SemaphoreType.DMA((chunks, 6)), pltpu.SemaphoreType.DMA((chunks,))],
        compiler_params=pltpu.CompilerParams(vmem_limit_bytes=VMEM),
        cost_estimate=_estimate(20 * x.size, x, dy, mine, other),
    )(ids, gain, x, dy, mine, other, far_h, left_l, right_l)


def _total_kernel(part, out, all_s, ssem, rsem):
    dp, me = lax.axis_index("dp"), lax.axis_index("tp")
    peers = [(dp, lax.rem(me + n, 4)) for n in range(1, 4)]
    barrier = pltpu.get_barrier_semaphore()
    for peer in peers:
        pl.semaphore_signal(barrier, inc=1, device_id=peer, device_id_type=pl.DeviceIdType.MESH)
    all_s[me] = part[...]
    pl.semaphore_wait(barrier, 3)
    copies = [pltpu.make_async_remote_copy(src_ref=part, dst_ref=all_s.at[me], send_sem=ssem.at[n], recv_sem=rsem.at[n],
                                           device_id=peer, device_id_type=pl.DeviceIdType.MESH) for n, peer in enumerate(peers)]
    for copy in copies:
        copy.start()
    for copy in copies:
        copy.wait()
    out[...] = (all_s[0] + all_s[1]) + (all_s[2] + all_s[3])


def total(part):
    vmem = pl.BlockSpec(memory_space=pltpu.VMEM)
    return pl.pallas_call(
        _total_kernel,
        in_specs=[vmem],
        out_specs=vmem,
        out_shape=_sds(part.shape, part.dtype),
        scratch_shapes=[pltpu.VMEM((4, *part.shape), part.dtype), pltpu.SemaphoreType.DMA((3,)), pltpu.SemaphoreType.DMA((3,))],
        compiler_params=pltpu.CompilerParams(collective_id=1, has_side_effects=True),
        cost_estimate=_estimate(4 * part.size, part),
    )(part)


def solution(mesh):
    half = HEAD // 2
    angle = np.arange(4 * BLOCK, dtype=np.float32)[:, None] * np.float32(THETA) ** (-np.arange(half, dtype=np.float32) / np.float32(half))
    table = np.concatenate([np.cos(angle), np.sin(angle)], 1)

    def send(a, pairs):
        return lax.ppermute(a, "tp", pairs)

    def body(x, dy, gain, wq, wk, wv, wo):
        me = lax.axis_index("tp").astype(jnp.int32)
        core, chip = me % 2, me // 2
        ids = jnp.stack([me, core, chip, 1 - chip, 2 * (1 - chip) + 1, 2 * (1 - chip)])
        a0, a1, a2, a3, y1, yr, yf, seen, dq, dkv, _, sum_l, far_h, mine, other = to_gradients(
            x, dy, gain, wq, wk, wv, wo, table)
        right_l, left_l = send(sum_l, [(0, 2), (2, 0)]), send(sum_l, [(1, 2), (3, 0)])
        dq, dkv = dq.reshape(4 * BLOCK, -1), dkv.reshape(4 * BLOCK, -1)
        dwo, dwq, dwk, dwv = weight_grads(ids, seen, dy, y1, yr, yf, (a0, a1, a2, a3), dq, dkv)
        dx, dgain = finish(ids, x, dy, gain, mine, other, far_h, left_l, right_l)
        dgain = total(dgain)
        return dx, dgain, dwq, dwk, dwv, dwo

    tokens, columns = P(("dp", "tp"), None), P(None, "tp")
    return jax.shard_map(
        body,
        mesh=mesh,
        in_specs=(tokens, tokens, P(None), columns, columns, columns, P("tp", None)),
        out_specs=(tokens, P("dp", None), P("dp", "tp"), P("dp", "tp"), P("dp", "tp"), P(("dp", "tp"), None)),
        check_vma=False,
    )
```

```python
import jax
import jax.numpy as jnp
import numpy as np
from jax import lax
from jax.experimental import pallas as pl
from jax.experimental.pallas import tpu as pltpu

from jax.sharding import PartitionSpec as P

NEG = -1e30
LOG2E = 1.4426950408889634
VMEM = 67043328
HEAD = 128
THETA = 10000
BLOCK = 256


def _estimate(flops, *arrays):
    return pl.CostEstimate(flops=flops, transcendentals=0, bytes_accessed=sum(a.size * a.dtype.itemsize for a in arrays))


def _sds(shape, dtype=jnp.bfloat16):
    return jax.ShapeDtypeStruct(shape, dtype)


ANY = pl.BlockSpec(memory_space=pl.ANY)


def _dot(a, b, ca, cb):
    return lax.dot_general(a, b, (((ca,), (cb,)), ((), ())), preferred_element_type=jnp.float32)


def _nt(a, b):
    return _dot(a, b, 1, 1)


def _turn(t, table, back=False):
    swapped = pltpu.roll(table, HEAD // 2, 1)
    low = lax.broadcasted_iota(jnp.int32, table.shape, 1) < HEAD // 2
    cos, sin = jnp.where(low, table, swapped), jnp.where(low, -swapped, table)
    turn = pltpu.roll(t, HEAD // 2, 1) * sin
    return t * cos - turn if back else t * cos + turn


def _causal():
    shape = (BLOCK, 2 * BLOCK)
    return lax.rem(lax.broadcasted_iota(jnp.int32, shape, 1), BLOCK) >= lax.broadcasted_iota(jnp.int32, shape, 0)


def _rows(block, size=BLOCK):
    return pl.ds(pl.multiple_of(block * size, size), size)


def _loop(first, last, body):
    lax.fori_loop(first, last, lambda i, _: body(i), None)


def _main_kernel(gain, table, x, dy, wq, wk, wv, wo,
                 a0_o, a1_o, a2_o, a3_o, y1_o, yr_o, yf_o, seen_o, dq_o, dkv_o, suml_o, far_o, base_o,
                 w_s, wo_s, st, qkv_s, do_s, o_s, lse_s, top_s, mix_s, dq_s, dk_s, dv_s, dqkv_s, own_s, give_s, got_s, keep_s,
                 lsem, ssem, rsem):
    dp, me = lax.axis_index("dp"), lax.axis_index("tp")
    core, chip = lax.rem(me, 2), lax.div(me, 2)
    beside, across = (dp, me + 1 - 2 * core), (dp, lax.rem(me + 2, 4))
    far = 1 - chip
    d = x.shape[1]
    half, part = d // 2, BLOCK // 2
    scale = HEAD**-0.5
    e = scale * LOG2E
    cols = 2 * BLOCK
    nh, kv = do_s.shape[0], dk_s.shape[0]
    MESH = pl.DeviceIdType.MESH

    barrier = pltpu.get_barrier_semaphore()
    for peer in range(1, 4):
        pl.semaphore_signal(barrier, inc=1, device_id=(dp, lax.rem(me + peer, 4)), device_id_type=MESH)
    pl.semaphore_wait(barrier, 3)

    used = [0, 0]

    def local(src, dst):
        copy = pltpu.make_async_copy(src, dst, lsem.at[used[0]])
        used[0] += 1
        copy.start()
        return copy

    def away(src, dst, to, at):
        return pltpu.make_async_remote_copy(src_ref=src, dst_ref=dst, send_sem=ssem.at[at], recv_sem=rsem.at[at], device_id=to,
                                            device_id_type=MESH)

    def remote(src, dst, to):
        copy = away(src, dst, to, used[1])
        used[1] += 1
        copy.start()
        return copy

    quarter = part // 2
    parts = [pl.ds(j * quarter, quarter) for j in range(4)]
    y1 = remote(dy, y1_o, beside)
    xs = [local(x.at[r], st.at[0, r]) for r in parts]
    nq, nk = wq.shape[1], wk.shape[1]
    wo_in = local(wo, wo_s)
    w_in = [local(w, w_s.at[:, pl.ds(at, w.shape[1])]) for w, at in ((wq, 0), (wk, nq), (wv, nq + nk))]
    far_a, near_a, ready = [], [], []

    def leave(j):
        ready[j].wait()
        far_a.append(remote(a0_o.at[parts[j]], a2_o.at[parts[j]], across))
        near_a.append(remote(a0_o.at[parts[j]], a1_o.at[parts[j]], beside))

    for j in range(4):
        xs[j].wait()

        def norm(i):
            rows = pl.ds(pl.multiple_of(j * quarter + i * 16, 16), 16)
            wide = st[0, rows, :].astype(jnp.float32)
            inv = lax.rsqrt(jnp.mean(wide * wide, -1, keepdims=True) + 1e-6)
            st[1, rows, :] = (wide * inv * gain[...].astype(jnp.float32)[None, :]).astype(jnp.bfloat16)

        _loop(0, quarter // 16, norm)
        ready.append(local(st.at[1, parts[j]], a0_o.at[parts[j]]))
        if j:
            leave(j - 1)
    leave(3)

    y1.wait_recv()
    first, second = pl.ds(0, half), pl.ds(half, half)
    hl = used[1]
    on = hl + 4
    tiles = d // WIDE
    gv = hl + 8
    across_h = gv + tiles
    own_other = across_h + tiles
    used[1] += 8 + 3 * tiles

    def over(src, i, r):
        rows = _rows(r, part)
        return away(src.at[rows], yr_o.at[i, rows], across, hl + 2 * i + r)

    @pl.when(core == 1)
    def _():
        for i, src in enumerate((dy, y1_o)):
            for r in range(2):
                over(src.at[:, first], i, r).start()

    @pl.when(core == 0)
    def _():
        for i, src in enumerate((y1_o, dy)):
            for r in range(2):
                over(src.at[:, second], i, r).start()

    y_in = [local(dy, st.at[0]), local(y1_o, st.at[1])]
    dk_s[...] = jnp.zeros_like(dk_s)
    dv_s[...] = jnp.zeros_like(dv_s)

    def dseen(slot, block):
        def tile(n):
            got = _nt(st[slot], wo_s[_rows(n, 4 * HEAD), :]).astype(jnp.bfloat16)
            for h in range(4):
                do_s[4 * n + h, _rows(block), :] = got[:, h * HEAD : (h + 1) * HEAD]

        _loop(0, nh // 4, tile)

    def project(slot, upper, lower):
        def tile(n):
            got = jnp.dot(st[slot], w_s[:, _rows(n, 4 * HEAD)], preferred_element_type=jnp.float32).astype(jnp.bfloat16)
            for p, place in enumerate((upper, lower)):
                rows = _rows(place, part)
                for h in range(4):
                    t = got[p * part : (p + 1) * part, h * HEAD : (h + 1) * HEAD].astype(jnp.float32)
                    t = jnp.where(n < (nq + nk) // (4 * HEAD), _turn(t, table[rows, :]), t)
                    qkv_s[4 * n + h, rows, :] = t.astype(jnp.bfloat16)

        _loop(0, w_s.shape[1] // (4 * HEAD), tile)

    wo_in.wait()
    for slot, block in ((0, me), (1, 2 * chip + 1 - core)):
        y_in[slot].wait()
        dseen(slot, block)
    a_in = local(a0_o, st.at[0])
    for w in w_in:
        w.wait()
    a_in.wait()
    project(0, 2 * me, 2 * me + 1)
    for c in near_a:
        c.wait_recv()
    local(a1_o, st.at[1]).wait()
    other = 2 * chip + 1 - core
    project(1, 2 * other, 2 * other + 1)

    def query(i, b):
        return qkv_s[pl.ds(2 * i, 2), _rows(b), :].reshape(cols, HEAD)

    def look(b, slot, start, stop, diagonal):
        qs = [query(i, b) for i in range(kv)]

        def block(j, masked):
            scores = [_nt(qkv_s[nh + i, _rows(j), :], qs[i]) for i in range(kv)]
            for i, s in enumerate(scores):
                at = slot * kv + i
                if masked:
                    s = jnp.where(_causal(), s, 2 * NEG)
                old = top_s[at]
                top = jnp.maximum(old, s.max(axis=0, keepdims=True))
                top_s[at] = top
                p = jnp.exp2((s - top) * e).astype(jnp.bfloat16)
                values = jnp.concatenate([qkv_s[nh + kv + i, _rows(j), :].T, jnp.ones((8, BLOCK), jnp.bfloat16)], axis=0)
                mix_s[at] = mix_s[at] * jnp.exp2((old - top) * e) + _dot(values, p, 1, 0)

        _loop(start, stop, lambda j: block(j, False))
        if diagonal:
            block(b, True)

    def begin():
        top_s[...] = jnp.full_like(top_s, NEG)
        mix_s[...] = jnp.zeros_like(mix_s)

    def end(b, slot):
        for i in range(kv):
            at = slot * kv + i
            total = mix_s[at, HEAD : HEAD + 1]
            got = (mix_s[at, :HEAD] * (1 / total)).T.astype(jnp.bfloat16)
            for h in range(2):
                o_s[2 * i + h, _rows(b), :] = got[h * BLOCK : (h + 1) * BLOCK]
            lse_s[kv * b + i] = (top_s[at] * scale + jnp.log(total)) * LOG2E

    def near(b):
        look(2 * chip + b, b, 2 * chip, 2 * chip + b, True)

    def rest(b):
        look(2 * chip + b, b, 0, 2 * chip, False)
        end(2 * chip + b, b)

    def distant(b):
        look(2 * far + b, b, 0, 2 * far + b, True)
        end(2 * far + b, b)

    begin()
    _loop(0, 2, near)

    for j in range(2):
        onward, loads = [], []
        for n in range(2):
            far_a[2 * j + n].wait_recv()
            rows = parts[2 * j + n]
            onward.append(remote(a2_o.at[rows], a3_o.at[rows], beside))
            loads.append(local(a2_o.at[rows], st.at[j, parts[n]]))
        for n in range(2):
            onward[n].wait_recv()
            loads.append(local(a3_o.at[parts[2 * j + n]], st.at[j, parts[2 + n]]))
        for copy in loads:
            copy.wait()
        project(j, 2 * (2 * far + core) + j, 2 * (2 * far + 1 - core) + j)
        for copy in onward:
            copy.wait_send()
    _loop(0, 2, rest)
    begin()
    _loop(0, 2, distant)
    seen_out = local(o_s, seen_o)

    def backward(b, to, place):
        def pair(g):
            dq_s[...] = jnp.zeros_like(dq_s)
            qs = [query(2 * g + i, b) for i in range(2)]
            dos = [do_s[pl.ds(4 * g + 2 * i, 2), _rows(b), :].reshape(cols, HEAD) for i in range(2)]
            outs = [o_s[pl.ds(4 * g + 2 * i, 2), _rows(b), :].reshape(cols, HEAD) for i in range(2)]
            deltas = [(y.astype(jnp.float32) * o.astype(jnp.float32)).T.sum(0, keepdims=True) for y, o in zip(dos, outs)]

            def block(j, masked):
                scores = [_nt(qkv_s[nh + 2 * g + i, _rows(j), :], qs[i]) for i in range(2)]
                dps = [_nt(qkv_s[nh + kv + 2 * g + i, _rows(j), :], dos[i]) for i in range(2)]
                for i in range(2):
                    at = 2 * g + i
                    p = jnp.exp2(scores[i] * e - lse_s[kv * b + at])
                    if masked:
                        p = jnp.where(_causal(), p, 0.0)
                    ds = (p * (dps[i] - deltas[i])).astype(jnp.bfloat16)
                    dv_s[at, _rows(j), :] += _dot(p.astype(jnp.bfloat16), dos[i], 1, 0)
                    dk_s[at, _rows(j), :] += _dot(ds, qs[i], 1, 0)
                    dq_s[i] += _dot(qkv_s[nh + at, _rows(j), :].T, ds, 1, 0)

            _loop(0, b, lambda j: block(j, False))
            block(b, True)
            for i in range(2):
                got = (dq_s[i] * scale).T
                for h in range(2):
                    t = got[h * BLOCK : (h + 1) * BLOCK].astype(jnp.bfloat16).astype(jnp.float32)
                    t = _turn(t, table[_rows(b), :], True)
                    to[_rows(place), _rows(4 * g + 2 * i + h, HEAD)] = t.astype(jnp.bfloat16)

        _loop(0, kv // 2, pair)

    loop_sems = used[0]
    used[0] += 10 + d // WIDE

    def loose(src, dst, at):
        return pltpu.make_async_copy(src, dst, lsem.at[loop_sems + at])

    queries = pl.ds(0, nq)

    def slot_of(i):
        return lax.rem(i + core + 1, 2)

    def own_out(i):
        return loose(own_s.at[_rows(slot_of(i)), queries], dq_o.at[i], 8 + i)

    def own(i):
        backward(2 * chip + i, own_s, slot_of(i))
        own_out(i).start()

    _loop(0, 2, own)

    def turn_back(b, at, to, place, sem):
        rows = _rows(place)
        for n in range(kv):
            t = _turn((dk_s[n, _rows(b), :] * scale).astype(jnp.bfloat16).astype(jnp.float32), table[_rows(b), :], True)
            to[rows, nq + n * HEAD : nq + (n + 1) * HEAD] = t.astype(jnp.bfloat16)
            to[rows, nq + nk + n * HEAD : nq + nk + (n + 1) * HEAD] = dv_s[n, _rows(b), :].astype(jnp.bfloat16)
        copy = loose(to.at[rows, pl.ds(nq, 2 * nk)], dkv_o.at[at], sem)
        copy.start()
        return copy

    slots = 3

    def tile(n):
        return _rows(n, WIDE)

    def slot(n):
        return _rows(lax.rem(n, slots), WIDE)

    def give_out(n):
        return away(give_s.at[:, slot(n)], got_s.at[:, tile(n)], beside, gv + n)

    def sum_away(n):
        return away(got_s.at[:, tile(n)], far_o.at[:, tile(n)], across, across_h + n)

    def low_out():
        return loose(got_s, suml_o, 5)

    def remote_block(i):
        b = 2 * far + 1 - i
        mine, others = _rows(1 - core, half), _rows(core, half)
        onward, loads = [], []
        for r in range(2):
            rows = _rows(r, part)
            over(dy.at[:, first], i, r).wait_recv()
            onward.append(away(yr_o.at[i, rows], yf_o.at[i, rows], beside, on + 2 * i + r))
            onward[r].start()
            loads.append(loose(yr_o.at[i, rows], st.at[i, rows, mine], 1 + r))
            loads[r].start()
        for copy in loads:
            copy.wait()

        def near_half(n):
            keep_s[:, _rows(n, 4 * HEAD)] = _nt(st[i, :, mine], wo_s[_rows(n, 4 * HEAD), mine])

        def far_half(n):
            got = keep_s[:, _rows(n, 4 * HEAD)] + _nt(st[i, :, others], wo_s[_rows(n, 4 * HEAD), others])
            for h in range(4):
                do_s[4 * n + h, _rows(b), :] = got[:, h * HEAD : (h + 1) * HEAD].astype(jnp.bfloat16)

        _loop(0, nh // 4, near_half)
        for r in range(2):
            rows = _rows(r, part)
            onward[r].wait_recv()
            loads.append(loose(yf_o.at[i, rows], st.at[i, rows, others], 6 + r))
            loads[2 + r].start()
        for copy in loads[2:]:
            copy.wait()
        _loop(0, nh // 4, far_half)
        backward(b, dqkv_s, 0)
        q_out = loose(dqkv_s.at[:, queries], dq_o.at[2 + i], 3)
        q_out.start()
        kv_out = turn_back(b, 2 + i, dqkv_s, 0, 4)

        def term(n):
            return _nt(dqkv_s[...], w_s[tile(n), :])

        def give(n):
            @pl.when(n >= slots)
            def _():
                give_out(n - slots).wait_send()

            give_s[:, slot(n)] = term(n).astype(jnp.bfloat16)
            give_out(n).start()

        def settle(m, more=None):
            give_out(m).wait_recv()
            got = None if more is None else more()
            got_s[:, tile(m)] = (keep_s[:, slot(m)] + got_s[:, tile(m)].astype(jnp.float32)).astype(jnp.bfloat16)
            if more is not None:
                keep_s[:, slot(m + 2)] = got

            @pl.when(i == 0)
            def _():
                sum_away(m).start()

        def keep():
            def first(n):
                keep_s[:, slot(n)] = term(n)

            _loop(0, 2, first)
            _loop(0, tiles - 2, lambda m: settle(m, lambda: term(m + 2)))
            _loop(tiles - 2, tiles, settle)

        @pl.when(core == i)
        def _():
            _loop(0, tiles, give)

        @pl.when(core == 1 - i)
        def _():
            keep()

            @pl.when(i == 1)
            def _():
                low_out().start()

        for copy in onward:
            copy.wait_send()
        q_out.wait()
        kv_out.wait()

    _loop(0, 2, remote_block)
    outs = [turn_back(2 * chip + place, place, own_s, at, 6 + at) for at, place in enumerate((1 - core, core))]
    for n in range(tiles - slots, tiles):
        give_out(n).wait_send()

    def other_out(n):
        return away(give_s.at[:, slot(n)], st.at[0, :, tile(n)], beside, own_other + n)

    def base_out(n):
        return pltpu.make_async_copy(keep_s.at[:, slot(n)], base_o.at[:, tile(n)], lsem.at[loop_sems + 10 + n])

    def own_term(n):
        return _nt(own_s[...], w_s[tile(n), :])

    def put(n, got):
        give_s[:, slot(n)] = got[:BLOCK].astype(jnp.bfloat16)
        keep_s[:, slot(n)] = got[BLOCK:]
        other_out(n).start()

    def own_settle(m, more):
        n = m + 2

        @pl.when((n >= slots) & (n < tiles))
        def _():
            other_out(n - slots).wait_send()
            base_out(n - slots).wait()

        other_out(m).wait_recv()
        got = own_term(n) if more else None
        keep_s[:, slot(m)] += st[0, :, tile(m)].astype(jnp.float32)
        base_out(m).start()
        if more:
            put(n, got)

    _loop(0, 2, lambda n: put(n, own_term(n)))
    _loop(0, tiles - 2, lambda m: own_settle(m, True))
    _loop(tiles - 2, tiles, lambda m: own_settle(m, False))
    for n in range(tiles - slots, tiles):
        other_out(n).wait_send()
        base_out(n).wait()
    for copy in outs:
        copy.wait()
    for i in range(2):
        own_out(i).wait()
    seen_out.wait()
    for c in (y1, *far_a, *near_a):
        c.wait_send()
    for n in range(4):
        over(dy.at[:, first], n // 2, n % 2).wait_send()

    @pl.when(core == 0)
    def _():
        low_out().wait()

    @pl.when(core == 1)
    def _():
        for n in range(tiles):
            sum_away(n).wait()


WIDE = 768


def to_gradients(x, dy, gain, wq, wk, wv, wo, table):
    _, d = x.shape
    nq, nk = wq.shape[1], wk.shape[1]
    nh, kv = nq // HEAD, nk // HEAD
    tokens = 4 * BLOCK
    f32, low = jnp.float32, jnp.bfloat16
    whole, halves = _sds((BLOCK, d)), _sds((2, BLOCK, d // 2))
    vmem = pl.BlockSpec(memory_space=pltpu.VMEM)
    shapes = [whole] * 5 + [halves] * 2 + [
        _sds((nh, tokens, HEAD)), _sds((4, BLOCK, nq)), _sds((4, BLOCK, 2 * nk)), whole,
        whole, _sds((BLOCK, d), f32)]
    return pl.pallas_call(
        _main_kernel,
        in_specs=[vmem] * 2 + [ANY] * 6,
        out_specs=[ANY] * len(shapes),
        out_shape=shapes,
        scratch_shapes=[
            pltpu.VMEM((d, nq + 2 * nk), low), pltpu.VMEM((nq, d), low), pltpu.VMEM((2, BLOCK, d), low),
            pltpu.VMEM((nh + 2 * kv, tokens, HEAD), low), pltpu.VMEM((nh, tokens, HEAD), low), pltpu.VMEM((nh, tokens, HEAD), low),
            pltpu.VMEM((4 * kv, 1, 2 * BLOCK), f32), pltpu.VMEM((2 * kv, 1, 2 * BLOCK), f32),
            pltpu.VMEM((2 * kv, HEAD + 8, 2 * BLOCK), f32), pltpu.VMEM((2, HEAD, 2 * BLOCK), f32), pltpu.VMEM((kv, tokens, HEAD), f32),
            pltpu.VMEM((kv, tokens, HEAD), f32), pltpu.VMEM((BLOCK, nq + 2 * nk), low), pltpu.VMEM((2 * BLOCK, nq + 2 * nk), low),
            pltpu.VMEM((BLOCK, d // 2), low), pltpu.VMEM((BLOCK, d), low), pltpu.VMEM((BLOCK, d // 2), f32),
            *[pltpu.SemaphoreType.DMA((64,))] * 3],
        compiler_params=pltpu.CompilerParams(vmem_limit_bytes=VMEM, collective_id=0, has_side_effects=True),
        cost_estimate=_estimate(2 * tokens * d * (4 * nq + 4 * nk), wq, wk, wv, wo),
    )(gain, table, x, dy, wq, wk, wv, wo)


def _grads_kernel(seen, y0, y1, yr, yf, a0, a1, a2, a3, dq, dkv, dwo, oq, ok, ov,
                  seen_s, t_s, in_s, dq_s, dkv_s, wo_s, w_s, sem, in_sem, out_sem):
    me = lax.axis_index("tp")
    core, chip = lax.rem(me, 2), lax.div(me, 2)
    far = 1 - chip
    steps = dwo.shape[1] // WIDE
    half = steps // 2
    nq, nk = oq.shape[1], ok.shape[1]

    def load(src, slot, row, n):
        return pltpu.make_async_copy(src, in_s.at[slot, _rows(row)], in_sem.at[slot, n])

    def dy_loads(n, slot):
        at = _rows(n, WIDE)
        return [load(y.at[:, at], slot, i, i) for i, y in enumerate((y0, y1))]

    def far_loads(y, n, slot):
        at = _rows(lax.rem(n, half), WIDE)
        return [load(y.at[i, :, at], slot, 2 + i, 2 + i) for i in range(2)]

    def a_loads(n, slot):
        at = _rows(n, WIDE)
        places = (core, 1 - core, 3 - core, 2 + core)
        return [load(a.at[:, at], slot, place, i) for i, (a, place) in enumerate(zip((a0, a1, a2, a3), places))]

    def fetch(m):
        slot = lax.rem(m, 2)

        @pl.when(m < steps)
        def _():
            for copy in dy_loads(m, slot):
                copy.start()

            @pl.when(lax.div(m, half) == 1 - core)
            def _():
                for copy in far_loads(yr, m, slot):
                    copy.start()

            @pl.when(lax.div(m, half) == core)
            def _():
                for copy in far_loads(yf, m, slot):
                    copy.start()

        @pl.when((m >= steps) & (m < 2 * steps))
        def _():
            for copy in a_loads(m - steps, slot):
                copy.start()

    def landed(slot):
        for copy in a_loads(0, slot):
            copy.wait()

    first = pltpu.make_async_copy(seen, seen_s, sem.at[0])
    first.start()
    fetch(0)
    fetch(1)
    later = [pltpu.make_async_copy(a, b, sem.at[n]) for n, a, b in ((1, dq, dq_s), (2, dkv, dkv_s))]
    for copy in later:
        copy.start()
    first.wait()
    blocks = (me, 2 * chip + 1 - core, 2 * far + 1, 2 * far)
    for h in range(seen.shape[0]):
        rows = jnp.concatenate([seen_s[h, _rows(b), :] for b in blocks], axis=0)
        t_s[h * HEAD : (h + 1) * HEAD, :] = rows.T

    def dwo_out(n):
        slot = lax.rem(n, 2)
        return pltpu.make_async_copy(wo_s.at[slot], dwo.at[:, _rows(n, WIDE)], out_sem.at[slot, 0])

    def dw_outs(n):
        slot = lax.rem(n, 2)
        parts = ((oq, 0), (ok, nq), (ov, nq + nk))
        return [pltpu.make_async_copy(w_s.at[slot, :, pl.ds(at, o.shape[1])], o.at[_rows(n, WIDE)], out_sem.at[slot, 1 + i])
                for i, (o, at) in enumerate(parts)]

    def by_wo(n):
        slot = lax.rem(n, 2)
        landed(slot)

        @pl.when(n >= 2)
        def _():
            dwo_out(n - 2).wait()

        wo_s[slot] = jnp.dot(t_s[...], in_s[slot], preferred_element_type=jnp.float32).astype(jnp.bfloat16)
        dwo_out(n).start()
        fetch(n + 2)

    def by_w(n):
        slot = lax.rem(n, 2)
        landed(slot)

        @pl.when(n >= 2)
        def _():
            for copy in dw_outs(n - 2):
                copy.wait()

        at = in_s[slot].T
        w_s[slot, :, :nq] = jnp.dot(at, dq_s[...], preferred_element_type=jnp.float32).astype(jnp.bfloat16)
        w_s[slot, :, nq:] = jnp.dot(at, dkv_s[...], preferred_element_type=jnp.float32).astype(jnp.bfloat16)
        for copy in dw_outs(n):
            copy.start()
        fetch(steps + n + 2)

    _loop(0, steps, by_wo)
    for copy in later:
        copy.wait()
    _loop(0, steps, by_w)
    for n in (steps - 2, steps - 1):
        dwo_out(n).wait()
        for copy in dw_outs(n):
            copy.wait()


def weight_grads(seen, y0, y1, yr, yf, states, dq, dkv):
    d = y0.shape[1]
    nq, nk = dq.shape[1], dkv.shape[1] // 2
    low = jnp.bfloat16
    tokens = 4 * BLOCK
    return pl.pallas_call(
        _grads_kernel,
        in_specs=[ANY] * 11,
        out_specs=[ANY] * 4,
        scratch_shapes=[pltpu.VMEM(seen.shape, low), pltpu.VMEM((nq, tokens), low), pltpu.VMEM((2, tokens, WIDE), low),
                        pltpu.VMEM(dq.shape, low), pltpu.VMEM(dkv.shape, low), pltpu.VMEM((2, nq, WIDE), low),
                        pltpu.VMEM((2, WIDE, nq + 2 * nk), low), pltpu.SemaphoreType.DMA((3,)), pltpu.SemaphoreType.DMA((2, 4)),
                        pltpu.SemaphoreType.DMA((2, 4))],
        out_shape=[_sds((nq, d)), *[_sds((d, w)) for w in (nq, nk, nk)]],
        compiler_params=pltpu.CompilerParams(vmem_limit_bytes=VMEM),
        cost_estimate=_estimate(8 * BLOCK * d * 2 * (nq + nk), seen, y0, y1, yr, yf, *states, dq, dkv),
    )(seen, y0, y1, yr, yf, *states, dq, dkv)


def _finish_kernel(gain, x, dy, base, far_h, far_l, dx, dgain_ref, x_s, dy_s, base_s, far_s, out_s, sum_s, sem, out_sem):
    core = lax.rem(lax.axis_index("tp"), 2)
    rows, d = x.shape
    chunks = sem.shape[0]
    step = rows // chunks
    ahead = 3

    def loads(c, far):
        here = _rows(c, step)
        pairs = ((x, x_s), (dy, dy_s), (base, base_s), (far, far_s))
        return [pltpu.make_async_copy(a.at[here], b.at[here], sem.at[c, n]) for n, (a, b) in enumerate(pairs)]

    def start(c):
        for owner, far in enumerate((far_l, far_h)):
            @pl.when(core == owner)
            def _():
                for load in loads(c, far):
                    load.start()

    def result(c):
        return pltpu.make_async_copy(out_s.at[_rows(c, step)], dx.at[_rows(c, step)], out_sem.at[c])

    for c in range(ahead):
        start(c)
    sum_s[...] = jnp.zeros_like(sum_s)

    def chunk(c):
        for load in loads(c, far_l):
            load.wait()

        @pl.when(c + ahead < chunks)
        def _():
            start(c + ahead)

        here = _rows(c, step)
        wide = x_s[here, :].astype(jnp.float32)
        scale = lax.rsqrt(jnp.mean(wide * wide, -1, keepdims=True) + 1e-6)
        hat = wide * scale
        da = base_s[here, :] + far_s[here, :].astype(jnp.float32)
        sum_s[...] += (da * hat).reshape(step // 8, 8, d).sum(0)
        by_hat = da * gain[...].astype(jnp.float32)[None, :]
        by_x = scale * (by_hat - hat * jnp.mean(by_hat * hat, -1, keepdims=True))
        out_s[here, :] = (dy_s[here, :].astype(jnp.float32) + by_x).astype(jnp.bfloat16)
        result(c).start()

    _loop(0, chunks, chunk)
    dgain_ref[...] = sum_s[...].sum(0, keepdims=True)
    for c in range(chunks):
        result(c).wait()


def finish(x, dy, gain, base, far_h, far_l):
    rows, d = x.shape
    chunks = 8
    low, f32 = jnp.bfloat16, jnp.float32
    vmem = pl.BlockSpec(memory_space=pltpu.VMEM)
    return pl.pallas_call(
        _finish_kernel,
        in_specs=[vmem, *[ANY] * 5],
        out_specs=[ANY, vmem],
        out_shape=[_sds((rows, d)), _sds((1, d), f32)],
        scratch_shapes=[*[pltpu.VMEM((rows, d), t) for t in (low, low, f32, low, low)], pltpu.VMEM((8, d), f32),
                        pltpu.SemaphoreType.DMA((chunks, 4)), pltpu.SemaphoreType.DMA((chunks,))],
        compiler_params=pltpu.CompilerParams(vmem_limit_bytes=VMEM),
        cost_estimate=_estimate(20 * x.size, x, dy, base),
    )(gain, x, dy, base, far_h, far_l)


def _total_kernel(part, out, all_s, ssem, rsem):
    dp, me = lax.axis_index("dp"), lax.axis_index("tp")
    peers = [(dp, lax.rem(me + n, 4)) for n in range(1, 4)]
    barrier = pltpu.get_barrier_semaphore()
    for peer in peers:
        pl.semaphore_signal(barrier, inc=1, device_id=peer, device_id_type=pl.DeviceIdType.MESH)
    all_s[me] = part[...]
    pl.semaphore_wait(barrier, 3)
    copies = [pltpu.make_async_remote_copy(src_ref=part, dst_ref=all_s.at[me], send_sem=ssem.at[n], recv_sem=rsem.at[n],
                                           device_id=peer, device_id_type=pl.DeviceIdType.MESH) for n, peer in enumerate(peers)]
    for copy in copies:
        copy.start()
    for copy in copies:
        copy.wait()
    out[...] = (all_s[0] + all_s[1]) + (all_s[2] + all_s[3])


def total(part):
    vmem = pl.BlockSpec(memory_space=pltpu.VMEM)
    return pl.pallas_call(
        _total_kernel,
        in_specs=[vmem],
        out_specs=vmem,
        out_shape=_sds(part.shape, part.dtype),
        scratch_shapes=[pltpu.VMEM((4, *part.shape), part.dtype), pltpu.SemaphoreType.DMA((3,)), pltpu.SemaphoreType.DMA((3,))],
        compiler_params=pltpu.CompilerParams(collective_id=1, has_side_effects=True),
        cost_estimate=_estimate(4 * part.size, part),
    )(part)


def solution(mesh):
    half = HEAD // 2
    angle = np.arange(4 * BLOCK, dtype=np.float32)[:, None] * np.float32(THETA) ** (-np.arange(half, dtype=np.float32) / np.float32(half))
    table = np.concatenate([np.cos(angle), np.sin(angle)], 1)

    def send(a, pairs):
        return lax.ppermute(a, "tp", pairs)

    def body(x, dy, gain, wq, wk, wv, wo):
        a0, a1, a2, a3, y1, yr, yf, seen, dq, dkv, sum_l, far_h, base = to_gradients(
            x, dy, gain, wq, wk, wv, wo, table)
        far_l = send(sum_l, [(0, 2), (2, 0)])
        dq, dkv = dq.reshape(4 * BLOCK, -1), dkv.reshape(4 * BLOCK, -1)
        dwo, dwq, dwk, dwv = weight_grads(seen, dy, y1, yr, yf, (a0, a1, a2, a3), dq, dkv)
        dx, dgain = finish(x, dy, gain, base, far_h, far_l)
        dgain = total(dgain)
        return dx, dgain, dwq, dwk, dwv, dwo

    tokens, columns = P(("dp", "tp"), None), P(None, "tp")
    return jax.shard_map(
        body,
        mesh=mesh,
        in_specs=(tokens, tokens, P(None), columns, columns, columns, P("tp", None)),
        out_specs=(tokens, P("dp", None), P("dp", "tp"), P("dp", "tp"), P("dp", "tp"), P(("dp", "tp"), None)),
        check_vma=False,
    )
```

```python
import jax
import jax.numpy as jnp
import numpy as np
from jax import lax
from jax.experimental import pallas as pl
from jax.experimental.pallas import tpu as pltpu

from jax.sharding import PartitionSpec as P

NEG = -1e30
LOG2E = 1.4426950408889634
VMEM = 67043328
HEAD = 128
THETA = 10000
BLOCK = 256


def _estimate(flops, *arrays):
    return pl.CostEstimate(flops=flops, transcendentals=0, bytes_accessed=sum(a.size * a.dtype.itemsize for a in arrays))


def _sds(shape, dtype=jnp.bfloat16):
    return jax.ShapeDtypeStruct(shape, dtype)


ANY = pl.BlockSpec(memory_space=pl.ANY)


def _dot(a, b, ca, cb):
    return lax.dot_general(a, b, (((ca,), (cb,)), ((), ())), preferred_element_type=jnp.float32)


def _nt(a, b):
    return _dot(a, b, 1, 1)


def _turn(t, table, back=False):
    swapped = pltpu.roll(table, HEAD // 2, 1)
    low = lax.broadcasted_iota(jnp.int32, table.shape, 1) < HEAD // 2
    cos, sin = jnp.where(low, table, swapped), jnp.where(low, -swapped, table)
    turn = pltpu.roll(t, HEAD // 2, 1) * sin
    return t * cos - turn if back else t * cos + turn


def _causal():
    shape = (BLOCK, 2 * BLOCK)
    return lax.rem(lax.broadcasted_iota(jnp.int32, shape, 1), BLOCK) >= lax.broadcasted_iota(jnp.int32, shape, 0)


def _rows(block, size=BLOCK):
    return pl.ds(pl.multiple_of(block * size, size), size)


def _loop(first, last, body):
    lax.fori_loop(first, last, lambda i, _: body(i), None)


def _main_kernel(gain, table, x, dy, wq, wk, wv, wo,
                 a0_o, a1_o, a2_o, a3_o, y1_o, yr_o, yf_o, seen_o, dq_o, dkv_o, suml_o, far_o, base_o,
                 w_s, wo_s, st, qkv_s, do_s, o_s, lse_s, top_s, mix_s, dq_s, dk_s, dv_s, dqkv_s, own_s, give_s, got_s, keep_s,
                 lsem, ssem, rsem):
    dp, me = lax.axis_index("dp"), lax.axis_index("tp")
    core, chip = lax.rem(me, 2), lax.div(me, 2)
    beside, across = (dp, me + 1 - 2 * core), (dp, lax.rem(me + 2, 4))
    far = 1 - chip
    d = x.shape[1]
    half, part = d // 2, BLOCK // 2
    scale = HEAD**-0.5
    e = scale * LOG2E
    cols = 2 * BLOCK
    nh, kv = do_s.shape[0], dk_s.shape[0]
    MESH = pl.DeviceIdType.MESH

    barrier = pltpu.get_barrier_semaphore()
    for peer in range(1, 4):
        pl.semaphore_signal(barrier, inc=1, device_id=(dp, lax.rem(me + peer, 4)), device_id_type=MESH)

    used = [0, 0]

    def local(src, dst):
        copy = pltpu.make_async_copy(src, dst, lsem.at[used[0]])
        used[0] += 1
        copy.start()
        return copy

    def away(src, dst, to, at):
        return pltpu.make_async_remote_copy(src_ref=src, dst_ref=dst, send_sem=ssem.at[at], recv_sem=rsem.at[at], device_id=to,
                                            device_id_type=MESH)

    def remote(src, dst, to):
        copy = away(src, dst, to, used[1])
        used[1] += 1
        copy.start()
        return copy

    quarter = part // 2
    parts = [pl.ds(j * quarter, quarter) for j in range(4)]
    xs = [local(x.at[r], st.at[0, r]) for r in parts]
    nq, nk = wq.shape[1], wk.shape[1]
    wo_in = local(wo, wo_s)
    w_in = [local(w, w_s.at[:, pl.ds(at, w.shape[1])]) for w, at in ((wq, 0), (wk, nq), (wv, nq + nk))]
    far_a, near_a, kept_a = [], [], []
    y1 = None
    for j in range(4):
        xs[j].wait()

        def norm(i):
            rows = pl.ds(pl.multiple_of(j * quarter + i * 16, 16), 16)
            wide = st[0, rows, :].astype(jnp.float32)
            inv = lax.rsqrt(jnp.mean(wide * wide, -1, keepdims=True) + 1e-6)
            got_s[rows, :] = (wide * inv * gain[...].astype(jnp.float32)[None, :]).astype(jnp.bfloat16)

        _loop(0, quarter // 16, norm)
        if y1 is None:
            pl.semaphore_wait(barrier, 3)
            y1 = remote(dy, y1_o, beside)
        far_a.append(remote(got_s.at[parts[j]], a2_o.at[parts[j]], across))
        near_a.append(remote(got_s.at[parts[j]], a1_o.at[parts[j]], beside))
        kept_a.append(local(got_s.at[parts[j]], a0_o.at[parts[j]]))

    y1.wait_recv()
    first, second = pl.ds(0, half), pl.ds(half, half)
    hl = used[1]
    on = hl + 4
    tiles = d // WIDE
    gv = hl + 8
    across_h = gv + tiles
    own_other = across_h + tiles
    used[1] += 8 + 3 * tiles

    def over(src, i, r):
        rows = _rows(r, part)
        return away(src.at[rows], yr_o.at[i, rows], across, hl + 2 * i + r)

    @pl.when(core == 1)
    def _():
        for i, src in enumerate((dy, y1_o)):
            for r in range(2):
                over(src.at[:, first], i, r).start()

    @pl.when(core == 0)
    def _():
        for i, src in enumerate((y1_o, dy)):
            for r in range(2):
                over(src.at[:, second], i, r).start()

    y_in = [local(dy, st.at[0]), local(y1_o, st.at[1])]
    dk_s[...] = jnp.zeros_like(dk_s)
    dv_s[...] = jnp.zeros_like(dv_s)

    def dseen(slot, block):
        def tile(n):
            got = _nt(st[slot], wo_s[_rows(n, 4 * HEAD), :]).astype(jnp.bfloat16)
            for h in range(4):
                do_s[4 * n + h, _rows(block), :] = got[:, h * HEAD : (h + 1) * HEAD]

        _loop(0, nh // 4, tile)

    def project(a_ref, upper, lower):
        def tile(n):
            got = jnp.dot(a_ref[...], w_s[:, _rows(n, 4 * HEAD)], preferred_element_type=jnp.float32).astype(jnp.bfloat16)
            for p, place in enumerate((upper, lower)):
                rows = _rows(place, part)
                for h in range(4):
                    t = got[p * part : (p + 1) * part, h * HEAD : (h + 1) * HEAD].astype(jnp.float32)
                    t = jnp.where(n < (nq + nk) // (4 * HEAD), _turn(t, table[rows, :]), t)
                    qkv_s[4 * n + h, rows, :] = t.astype(jnp.bfloat16)

        _loop(0, w_s.shape[1] // (4 * HEAD), tile)

    wo_in.wait()
    for slot, block in ((0, me), (1, 2 * chip + 1 - core)):
        y_in[slot].wait()
        dseen(slot, block)
    for w in w_in:
        w.wait()
    project(got_s, 2 * me, 2 * me + 1)
    for c in near_a:
        c.wait_recv()
    local(a1_o, st.at[1]).wait()
    other = 2 * chip + 1 - core
    project(st.at[1], 2 * other, 2 * other + 1)

    def query(i, b):
        return qkv_s[pl.ds(2 * i, 2), _rows(b), :].reshape(cols, HEAD)

    def look(b, slot, start, stop, diagonal):
        qs = [query(i, b) for i in range(kv)]

        def block(j, masked):
            scores = [_nt(qkv_s[nh + i, _rows(j), :], qs[i]) for i in range(kv)]
            for i, s in enumerate(scores):
                at = slot * kv + i
                if masked:
                    s = jnp.where(_causal(), s, 2 * NEG)
                old = top_s[at]
                top = jnp.maximum(old, s.max(axis=0, keepdims=True))
                top_s[at] = top
                p = jnp.exp2((s - top) * e).astype(jnp.bfloat16)
                values = jnp.concatenate([qkv_s[nh + kv + i, _rows(j), :].T, jnp.ones((8, BLOCK), jnp.bfloat16)], axis=0)
                mix_s[at] = mix_s[at] * jnp.exp2((old - top) * e) + _dot(values, p, 1, 0)

        _loop(start, stop, lambda j: block(j, False))
        if diagonal:
            block(b, True)

    def begin():
        top_s[...] = jnp.full_like(top_s, NEG)
        mix_s[...] = jnp.zeros_like(mix_s)

    def end(b, slot):
        for i in range(kv):
            at = slot * kv + i
            total = mix_s[at, HEAD : HEAD + 1]
            got = (mix_s[at, :HEAD] * (1 / total)).T.astype(jnp.bfloat16)
            for h in range(2):
                o_s[2 * i + h, _rows(b), :] = got[h * BLOCK : (h + 1) * BLOCK]
            lse_s[kv * b + i] = (top_s[at] * scale + jnp.log(total)) * LOG2E

    def near(b):
        look(2 * chip + b, b, 2 * chip, 2 * chip + b, True)

    def rest(b):
        look(2 * chip + b, b, 0, 2 * chip, False)
        end(2 * chip + b, b)

    def distant(b):
        look(2 * far + b, b, 0, 2 * far + b, True)
        end(2 * far + b, b)

    begin()
    _loop(0, 2, near)

    for j in range(2):
        onward, loads = [], []
        for n in range(2):
            far_a[2 * j + n].wait_recv()
            rows = parts[2 * j + n]
            onward.append(remote(a2_o.at[rows], a3_o.at[rows], beside))
            loads.append(local(a2_o.at[rows], st.at[j, parts[n]]))
        for n in range(2):
            onward[n].wait_recv()
            loads.append(local(a3_o.at[parts[2 * j + n]], st.at[j, parts[2 + n]]))
        for copy in loads:
            copy.wait()
        project(st.at[j], 2 * (2 * far + core) + j, 2 * (2 * far + 1 - core) + j)
        for copy in onward:
            copy.wait_send()
    _loop(0, 2, rest)
    begin()
    _loop(0, 2, distant)
    seen_out = local(o_s, seen_o)

    def backward(b, to, place):
        def pair(g):
            dq_s[...] = jnp.zeros_like(dq_s)
            qs = [query(2 * g + i, b) for i in range(2)]
            dos = [do_s[pl.ds(4 * g + 2 * i, 2), _rows(b), :].reshape(cols, HEAD) for i in range(2)]
            outs = [o_s[pl.ds(4 * g + 2 * i, 2), _rows(b), :].reshape(cols, HEAD) for i in range(2)]
            deltas = [(y.astype(jnp.float32) * o.astype(jnp.float32)).T.sum(0, keepdims=True) for y, o in zip(dos, outs)]

            def block(j, masked):
                scores = [_nt(qkv_s[nh + 2 * g + i, _rows(j), :], qs[i]) for i in range(2)]
                dps = [_nt(qkv_s[nh + kv + 2 * g + i, _rows(j), :], dos[i]) for i in range(2)]
                for i in range(2):
                    at = 2 * g + i
                    p = jnp.exp2(scores[i] * e - lse_s[kv * b + at])
                    if masked:
                        p = jnp.where(_causal(), p, 0.0)
                    ds = (p * (dps[i] - deltas[i])).astype(jnp.bfloat16)
                    dv_s[at, _rows(j), :] += _dot(p.astype(jnp.bfloat16), dos[i], 1, 0)
                    dk_s[at, _rows(j), :] += _dot(ds, qs[i], 1, 0)
                    dq_s[i] += _dot(qkv_s[nh + at, _rows(j), :].T, ds, 1, 0)

            _loop(0, b, lambda j: block(j, False))
            block(b, True)
            for i in range(2):
                got = (dq_s[i] * scale).T
                for h in range(2):
                    t = got[h * BLOCK : (h + 1) * BLOCK].astype(jnp.bfloat16).astype(jnp.float32)
                    t = _turn(t, table[_rows(b), :], True)
                    to[_rows(place), _rows(4 * g + 2 * i + h, HEAD)] = t.astype(jnp.bfloat16)

        _loop(0, kv // 2, pair)

    loop_sems = used[0]
    used[0] += 10 + d // WIDE

    def loose(src, dst, at):
        return pltpu.make_async_copy(src, dst, lsem.at[loop_sems + at])

    queries = pl.ds(0, nq)

    def slot_of(i):
        return lax.rem(i + core + 1, 2)

    def own_out(i):
        return loose(own_s.at[_rows(slot_of(i)), queries], dq_o.at[i], 8 + i)

    def own(i):
        backward(2 * chip + i, own_s, slot_of(i))
        own_out(i).start()

    _loop(0, 2, own)

    def turn_back(b, at, to, place, sem):
        rows = _rows(place)
        for n in range(kv):
            t = _turn((dk_s[n, _rows(b), :] * scale).astype(jnp.bfloat16).astype(jnp.float32), table[_rows(b), :], True)
            to[rows, nq + n * HEAD : nq + (n + 1) * HEAD] = t.astype(jnp.bfloat16)
            to[rows, nq + nk + n * HEAD : nq + nk + (n + 1) * HEAD] = dv_s[n, _rows(b), :].astype(jnp.bfloat16)
        copy = loose(to.at[rows, pl.ds(nq, 2 * nk)], dkv_o.at[at], sem)
        copy.start()
        return copy

    slots = 3

    def tile(n):
        return _rows(n, WIDE)

    def slot(n):
        return _rows(lax.rem(n, slots), WIDE)

    def give_out(n):
        return away(give_s.at[:, slot(n)], got_s.at[:, tile(n)], beside, gv + n)

    def sum_away(n):
        return away(got_s.at[:, tile(n)], far_o.at[:, tile(n)], across, across_h + n)

    def low_out():
        return loose(got_s, suml_o, 5)

    def remote_block(i):
        b = 2 * far + 1 - i
        mine, others = _rows(1 - core, half), _rows(core, half)
        onward, loads = [], []
        for r in range(2):
            rows = _rows(r, part)
            over(dy.at[:, first], i, r).wait_recv()
            onward.append(away(yr_o.at[i, rows], yf_o.at[i, rows], beside, on + 2 * i + r))
            onward[r].start()
            loads.append(loose(yr_o.at[i, rows], st.at[i, rows, mine], 1 + r))
            loads[r].start()
        for copy in loads:
            copy.wait()

        def near_half(n):
            keep_s[:, _rows(n, 4 * HEAD)] = _nt(st[i, :, mine], wo_s[_rows(n, 4 * HEAD), mine])

        def far_half(n):
            got = keep_s[:, _rows(n, 4 * HEAD)] + _nt(st[i, :, others], wo_s[_rows(n, 4 * HEAD), others])
            for h in range(4):
                do_s[4 * n + h, _rows(b), :] = got[:, h * HEAD : (h + 1) * HEAD].astype(jnp.bfloat16)

        _loop(0, nh // 4, near_half)
        for r in range(2):
            rows = _rows(r, part)
            onward[r].wait_recv()
            loads.append(loose(yf_o.at[i, rows], st.at[i, rows, others], 6 + r))
            loads[2 + r].start()
        for copy in loads[2:]:
            copy.wait()
        _loop(0, nh // 4, far_half)
        backward(b, dqkv_s, 0)
        q_out = loose(dqkv_s.at[:, queries], dq_o.at[2 + i], 3)
        q_out.start()
        kv_out = turn_back(b, 2 + i, dqkv_s, 0, 4)

        def term(n):
            return _nt(dqkv_s[...], w_s[tile(n), :])

        def give(n):
            @pl.when(n >= slots)
            def _():
                give_out(n - slots).wait_send()

            give_s[:, slot(n)] = term(n).astype(jnp.bfloat16)
            give_out(n).start()

        def settle(m, more=None):
            give_out(m).wait_recv()
            got = None if more is None else more()
            got_s[:, tile(m)] = (keep_s[:, slot(m)] + got_s[:, tile(m)].astype(jnp.float32)).astype(jnp.bfloat16)
            if more is not None:
                keep_s[:, slot(m + 2)] = got

            @pl.when(i == 0)
            def _():
                sum_away(m).start()

        def keep():
            def first(n):
                keep_s[:, slot(n)] = term(n)

            _loop(0, 2, first)
            _loop(0, tiles - 2, lambda m: settle(m, lambda: term(m + 2)))
            _loop(tiles - 2, tiles, settle)

        @pl.when(core == i)
        def _():
            _loop(0, tiles, give)

        @pl.when(core == 1 - i)
        def _():
            keep()

            @pl.when(i == 1)
            def _():
                low_out().start()

        for copy in onward:
            copy.wait_send()
        q_out.wait()
        kv_out.wait()

    for c in kept_a:
        c.wait()
    for c in (*far_a, *near_a):
        c.wait_send()
    _loop(0, 2, remote_block)
    outs = [turn_back(2 * chip + place, place, own_s, at, 6 + at) for at, place in enumerate((1 - core, core))]
    for n in range(tiles - slots, tiles):
        give_out(n).wait_send()

    def other_out(n):
        return away(give_s.at[:, slot(n)], st.at[0, :, tile(n)], beside, own_other + n)

    def base_out(n):
        return pltpu.make_async_copy(keep_s.at[:, slot(n)], base_o.at[:, tile(n)], lsem.at[loop_sems + 10 + n])

    def own_term(n):
        return _nt(own_s[...], w_s[tile(n), :])

    def put(n, got):
        give_s[:, slot(n)] = got[:BLOCK].astype(jnp.bfloat16)
        keep_s[:, slot(n)] = got[BLOCK:]
        other_out(n).start()

    def own_settle(m, more):
        n = m + 2

        @pl.when((n >= slots) & (n < tiles))
        def _():
            other_out(n - slots).wait_send()
            base_out(n - slots).wait()

        other_out(m).wait_recv()
        got = own_term(n) if more else None
        keep_s[:, slot(m)] += st[0, :, tile(m)].astype(jnp.float32)
        base_out(m).start()
        if more:
            put(n, got)

    _loop(0, 2, lambda n: put(n, own_term(n)))
    _loop(0, tiles - 2, lambda m: own_settle(m, True))
    _loop(tiles - 2, tiles, lambda m: own_settle(m, False))
    for n in range(tiles - slots, tiles):
        other_out(n).wait_send()
        base_out(n).wait()
    for copy in outs:
        copy.wait()
    for i in range(2):
        own_out(i).wait()
    seen_out.wait()
    y1.wait_send()
    for n in range(4):
        over(dy.at[:, first], n // 2, n % 2).wait_send()

    @pl.when(core == 0)
    def _():
        low_out().wait()

    @pl.when(core == 1)
    def _():
        for n in range(tiles):
            sum_away(n).wait()


WIDE = 768


def to_gradients(x, dy, gain, wq, wk, wv, wo, table):
    _, d = x.shape
    nq, nk = wq.shape[1], wk.shape[1]
    nh, kv = nq // HEAD, nk // HEAD
    tokens = 4 * BLOCK
    f32, low = jnp.float32, jnp.bfloat16
    whole, halves = _sds((BLOCK, d)), _sds((2, BLOCK, d // 2))
    vmem = pl.BlockSpec(memory_space=pltpu.VMEM)
    shapes = [whole] * 5 + [halves] * 2 + [
        _sds((nh, tokens, HEAD)), _sds((4, BLOCK, nq)), _sds((4, BLOCK, 2 * nk)), whole,
        whole, _sds((BLOCK, d), f32)]
    return pl.pallas_call(
        _main_kernel,
        in_specs=[vmem] * 2 + [ANY] * 6,
        out_specs=[ANY] * len(shapes),
        out_shape=shapes,
        scratch_shapes=[
            pltpu.VMEM((d, nq + 2 * nk), low), pltpu.VMEM((nq, d), low), pltpu.VMEM((2, BLOCK, d), low),
            pltpu.VMEM((nh + 2 * kv, tokens, HEAD), low), pltpu.VMEM((nh, tokens, HEAD), low), pltpu.VMEM((nh, tokens, HEAD), low),
            pltpu.VMEM((4 * kv, 1, 2 * BLOCK), f32), pltpu.VMEM((2 * kv, 1, 2 * BLOCK), f32),
            pltpu.VMEM((2 * kv, HEAD + 8, 2 * BLOCK), f32), pltpu.VMEM((2, HEAD, 2 * BLOCK), f32), pltpu.VMEM((kv, tokens, HEAD), f32),
            pltpu.VMEM((kv, tokens, HEAD), f32), pltpu.VMEM((BLOCK, nq + 2 * nk), low), pltpu.VMEM((2 * BLOCK, nq + 2 * nk), low),
            pltpu.VMEM((BLOCK, d // 2), low), pltpu.VMEM((BLOCK, d), low), pltpu.VMEM((BLOCK, d // 2), f32),
            *[pltpu.SemaphoreType.DMA((64,))] * 3],
        compiler_params=pltpu.CompilerParams(vmem_limit_bytes=VMEM, collective_id=0, has_side_effects=True),
        cost_estimate=_estimate(2 * tokens * d * (4 * nq + 4 * nk), wq, wk, wv, wo),
    )(gain, table, x, dy, wq, wk, wv, wo)


def _grads_kernel(seen, y0, y1, yr, yf, a0, a1, a2, a3, dq, dkv, dwo, oq, ok, ov,
                  seen_s, t_s, in_s, dq_s, dkv_s, wo_s, w_s, sem, in_sem, out_sem):
    me = lax.axis_index("tp")
    core, chip = lax.rem(me, 2), lax.div(me, 2)
    far = 1 - chip
    steps = dwo.shape[1] // WIDE
    half = steps // 2
    nq, nk = oq.shape[1], ok.shape[1]

    def load(src, slot, row, n):
        return pltpu.make_async_copy(src, in_s.at[slot, _rows(row)], in_sem.at[slot, n])

    def dy_loads(n, slot):
        at = _rows(n, WIDE)
        return [load(y.at[:, at], slot, i, i) for i, y in enumerate((y0, y1))]

    def far_loads(y, n, slot):
        at = _rows(lax.rem(n, half), WIDE)
        return [load(y.at[i, :, at], slot, 2 + i, 2 + i) for i in range(2)]

    def a_loads(n, slot):
        at = _rows(n, WIDE)
        places = (core, 1 - core, 3 - core, 2 + core)
        return [load(a.at[:, at], slot, place, i) for i, (a, place) in enumerate(zip((a0, a1, a2, a3), places))]

    def fetch(m):
        slot = lax.rem(m, 2)

        @pl.when(m < steps)
        def _():
            for copy in dy_loads(m, slot):
                copy.start()

            @pl.when(lax.div(m, half) == 1 - core)
            def _():
                for copy in far_loads(yr, m, slot):
                    copy.start()

            @pl.when(lax.div(m, half) == core)
            def _():
                for copy in far_loads(yf, m, slot):
                    copy.start()

        @pl.when((m >= steps) & (m < 2 * steps))
        def _():
            for copy in a_loads(m - steps, slot):
                copy.start()

    def landed(slot):
        for copy in a_loads(0, slot):
            copy.wait()

    first = pltpu.make_async_copy(seen, seen_s, sem.at[0])
    first.start()
    fetch(0)
    first.wait()
    fetch(1)
    later = [pltpu.make_async_copy(a, b, sem.at[n]) for n, a, b in ((1, dq, dq_s), (2, dkv, dkv_s))]
    for copy in later:
        copy.start()
    blocks = (me, 2 * chip + 1 - core, 2 * far + 1, 2 * far)
    for h in range(seen.shape[0]):
        rows = jnp.concatenate([seen_s[h, _rows(b), :] for b in blocks], axis=0)
        t_s[h * HEAD : (h + 1) * HEAD, :] = rows.T

    def dwo_out(n):
        slot = lax.rem(n, 2)
        return pltpu.make_async_copy(wo_s.at[slot], dwo.at[:, _rows(n, WIDE)], out_sem.at[slot, 0])

    def dw_outs(n):
        slot = lax.rem(n, 2)
        parts = ((oq, 0), (ok, nq), (ov, nq + nk))
        return [pltpu.make_async_copy(w_s.at[slot, :, pl.ds(at, o.shape[1])], o.at[_rows(n, WIDE)], out_sem.at[slot, 1 + i])
                for i, (o, at) in enumerate(parts)]

    def by_wo(n):
        slot = lax.rem(n, 2)
        landed(slot)

        @pl.when(n >= 2)
        def _():
            dwo_out(n - 2).wait()

        wo_s[slot] = jnp.dot(t_s[...], in_s[slot], preferred_element_type=jnp.float32).astype(jnp.bfloat16)
        dwo_out(n).start()
        fetch(n + 2)

    def by_w(n):
        slot = lax.rem(n, 2)
        landed(slot)

        @pl.when(n >= 2)
        def _():
            for copy in dw_outs(n - 2):
                copy.wait()

        at = in_s[slot].T
        w_s[slot, :, :nq] = jnp.dot(at, dq_s[...], preferred_element_type=jnp.float32).astype(jnp.bfloat16)
        w_s[slot, :, nq:] = jnp.dot(at, dkv_s[...], preferred_element_type=jnp.float32).astype(jnp.bfloat16)
        for copy in dw_outs(n):
            copy.start()
        fetch(steps + n + 2)

    _loop(0, steps, by_wo)
    for copy in later:
        copy.wait()
    _loop(0, steps, by_w)
    for n in (steps - 2, steps - 1):
        dwo_out(n).wait()
        for copy in dw_outs(n):
            copy.wait()


def weight_grads(seen, y0, y1, yr, yf, states, dq, dkv):
    d = y0.shape[1]
    nq, nk = dq.shape[1], dkv.shape[1] // 2
    low = jnp.bfloat16
    tokens = 4 * BLOCK
    return pl.pallas_call(
        _grads_kernel,
        in_specs=[ANY] * 11,
        out_specs=[ANY] * 4,
        scratch_shapes=[pltpu.VMEM(seen.shape, low), pltpu.VMEM((nq, tokens), low), pltpu.VMEM((2, tokens, WIDE), low),
                        pltpu.VMEM(dq.shape, low), pltpu.VMEM(dkv.shape, low), pltpu.VMEM((2, nq, WIDE), low),
                        pltpu.VMEM((2, WIDE, nq + 2 * nk), low), pltpu.SemaphoreType.DMA((3,)), pltpu.SemaphoreType.DMA((2, 4)),
                        pltpu.SemaphoreType.DMA((2, 4))],
        out_shape=[_sds((nq, d)), *[_sds((d, w)) for w in (nq, nk, nk)]],
        compiler_params=pltpu.CompilerParams(vmem_limit_bytes=VMEM),
        cost_estimate=_estimate(8 * BLOCK * d * 2 * (nq + nk), seen, y0, y1, yr, yf, *states, dq, dkv),
    )(seen, y0, y1, yr, yf, *states, dq, dkv)


def _finish_kernel(gain, x, dy, base, far_h, far_l, dx, dgain_ref, x_s, dy_s, base_s, far_s, out_s, sum_s, sem, out_sem):
    core = lax.rem(lax.axis_index("tp"), 2)
    rows, d = x.shape
    chunks = sem.shape[0]
    step = rows // chunks
    ahead = 3

    def loads(c, far):
        here = _rows(c, step)
        pairs = ((x, x_s), (dy, dy_s), (base, base_s), (far, far_s))
        return [pltpu.make_async_copy(a.at[here], b.at[here], sem.at[c, n]) for n, (a, b) in enumerate(pairs)]

    def start(c):
        for owner, far in enumerate((far_l, far_h)):
            @pl.when(core == owner)
            def _():
                for load in loads(c, far):
                    load.start()

    def result(c):
        return pltpu.make_async_copy(out_s.at[_rows(c, step)], dx.at[_rows(c, step)], out_sem.at[c])

    for c in range(ahead):
        start(c)
    sum_s[...] = jnp.zeros_like(sum_s)

    def chunk(c):
        for load in loads(c, far_l):
            load.wait()

        @pl.when(c + ahead < chunks)
        def _():
            start(c + ahead)

        here = _rows(c, step)
        wide = x_s[here, :].astype(jnp.float32)
        scale = lax.rsqrt(jnp.mean(wide * wide, -1, keepdims=True) + 1e-6)
        hat = wide * scale
        da = base_s[here, :] + far_s[here, :].astype(jnp.float32)
        sum_s[...] += (da * hat).reshape(step // 8, 8, d).sum(0)
        by_hat = da * gain[...].astype(jnp.float32)[None, :]
        by_x = scale * (by_hat - hat * jnp.mean(by_hat * hat, -1, keepdims=True))
        out_s[here, :] = (dy_s[here, :].astype(jnp.float32) + by_x).astype(jnp.bfloat16)
        result(c).start()

    _loop(0, chunks, chunk)
    dgain_ref[...] = sum_s[...].sum(0, keepdims=True)
    for c in range(chunks):
        result(c).wait()


def finish(x, dy, gain, base, far_h, far_l):
    rows, d = x.shape
    chunks = 8
    low, f32 = jnp.bfloat16, jnp.float32
    vmem = pl.BlockSpec(memory_space=pltpu.VMEM)
    return pl.pallas_call(
        _finish_kernel,
        in_specs=[vmem, *[ANY] * 5],
        out_specs=[ANY, vmem],
        out_shape=[_sds((rows, d)), _sds((1, d), f32)],
        scratch_shapes=[*[pltpu.VMEM((rows, d), t) for t in (low, low, f32, low, low)], pltpu.VMEM((8, d), f32),
                        pltpu.SemaphoreType.DMA((chunks, 4)), pltpu.SemaphoreType.DMA((chunks,))],
        compiler_params=pltpu.CompilerParams(vmem_limit_bytes=VMEM),
        cost_estimate=_estimate(20 * x.size, x, dy, base),
    )(gain, x, dy, base, far_h, far_l)


def _total_kernel(part, out, all_s, ssem, rsem):
    dp, me = lax.axis_index("dp"), lax.axis_index("tp")
    peers = [(dp, lax.rem(me + n, 4)) for n in range(1, 4)]
    barrier = pltpu.get_barrier_semaphore()
    for peer in peers:
        pl.semaphore_signal(barrier, inc=1, device_id=peer, device_id_type=pl.DeviceIdType.MESH)
    all_s[me] = part[...]
    pl.semaphore_wait(barrier, 3)
    copies = [pltpu.make_async_remote_copy(src_ref=part, dst_ref=all_s.at[me], send_sem=ssem.at[n], recv_sem=rsem.at[n],
                                           device_id=peer, device_id_type=pl.DeviceIdType.MESH) for n, peer in enumerate(peers)]
    for copy in copies:
        copy.start()
    for copy in copies:
        copy.wait()
    out[...] = (all_s[0] + all_s[1]) + (all_s[2] + all_s[3])


def total(part):
    vmem = pl.BlockSpec(memory_space=pltpu.VMEM)
    return pl.pallas_call(
        _total_kernel,
        in_specs=[vmem],
        out_specs=vmem,
        out_shape=_sds(part.shape, part.dtype),
        scratch_shapes=[pltpu.VMEM((4, *part.shape), part.dtype), pltpu.SemaphoreType.DMA((3,)), pltpu.SemaphoreType.DMA((3,))],
        compiler_params=pltpu.CompilerParams(collective_id=1, has_side_effects=True),
        cost_estimate=_estimate(4 * part.size, part),
    )(part)


def solution(mesh):
    half = HEAD // 2
    angle = np.arange(4 * BLOCK, dtype=np.float32)[:, None] * np.float32(THETA) ** (-np.arange(half, dtype=np.float32) / np.float32(half))
    table = np.concatenate([np.cos(angle), np.sin(angle)], 1)

    def send(a, pairs):
        return lax.ppermute(a, "tp", pairs)

    def body(x, dy, gain, wq, wk, wv, wo):
        a0, a1, a2, a3, y1, yr, yf, seen, dq, dkv, sum_l, far_h, base = to_gradients(
            x, dy, gain, wq, wk, wv, wo, table)
        far_l = send(sum_l, [(0, 2), (2, 0)])
        dq, dkv = dq.reshape(4 * BLOCK, -1), dkv.reshape(4 * BLOCK, -1)
        dwo, dwq, dwk, dwv = weight_grads(seen, dy, y1, yr, yf, (a0, a1, a2, a3), dq, dkv)
        dx, dgain = finish(x, dy, gain, base, far_h, far_l)
        dgain = total(dgain)
        return dx, dgain, dwq, dwk, dwv, dwo

    tokens, columns = P(("dp", "tp"), None), P(None, "tp")
    return jax.shard_map(
        body,
        mesh=mesh,
        in_specs=(tokens, tokens, P(None), columns, columns, columns, P("tp", None)),
        out_specs=(tokens, P("dp", None), P("dp", "tp"), P("dp", "tp"), P("dp", "tp"), P(("dp", "tp"), None)),
        check_vma=False,
    )
```
